32 devices in a mesh: gx: 4 (over x, core), gy: 8 (over z, y).
Axes of the slice: x: 2, y: 2, z: 4, core: 2. Of those that a mesh axis runs over, the one named last changes fastest.
Arguments:
- normal_matrix: float32 [4096, 4096], P(('gx', 'gy')), may hold values from -1 to 4, as said below
- right_sides: float32 [4096, 32], P(('gx', 'gy')), may hold values from -6 to 6
- tile_order: int32 [32], replicated, may hold values from 0 to 31, as said below
- inner_order: int32 [32, 128], replicated, may hold values from 0 to 127, each once within a row
- block_lengths: int32 [16], replicated, may hold values from 1 to 3, as said below
Outputs:
- renumbered: float32 [4096, 4096], P(None, ('gx', 'gy'))
- solution: float32 [4096, 32], P(('gx', 'gy'))
The draws below stay inside these ranges and needn't reach their ends.
Inputs may be any that keep to these rules, and one draw needn't show every extreme that they name: `normal_matrix`: symmetric positive definite. `tile_order`: a permutation. `inner_order`: each row a permutation. `block_lengths`: the lengths sum to 32, and the largest is 3.
All inputs are finite; a program needn't handle non-finite values.
Results may differ from the reference program's by a relative error of at most 0.0003.
Values sent between devices are 32-bit elements; how exact they have to be, the bound alone decides.
No kernel may reach another device: no remote copies, remote signals or barrier semaphores. Data moves between devices by JAX's collectives and lax.ppermute only.
A program may use at most 128 MiB of HBM per device.

```python
import math
import jax
import jax.numpy as jnp
from jax import lax

TILE = 128
MOSTT = 3
ITERS = 1
TILES = 32
ORDER = 4096
BLOCKS = 16
RHS = 32


def order_and_lengths(key):
    tile_order = jax.random.permutation(jax.random.fold_in(key, 101), TILES).astype(jnp.int32)
    leading = [MOSTT] + [1] * (MOSTT - 2)
    remaining = BLOCKS - len(leading)
    paired_count = remaining // 2
    shifts = jax.random.randint(jax.random.fold_in(key, 103), (paired_count,), -1, 2, dtype=jnp.int32)
    paired = jnp.stack([2 - shifts, 2 + shifts], axis=1).reshape(-1).astype(jnp.int32)
    leftover = jnp.full((remaining - 2 * paired_count,), 2, jnp.int32)
    base = jnp.concatenate([jnp.array(leading, jnp.int32), paired, leftover])
    mixing = jax.random.permutation(jax.random.fold_in(key, 107), BLOCKS).astype(jnp.int32)
    lengths = jnp.take(base, mixing).astype(jnp.int32)
    return (tile_order, lengths)


def draw_tile_order(key, part):
    return order_and_lengths(key)[0]


def draw_block_lengths(key, part):
    return order_and_lengths(key)[1]


def draw_normal_matrix(key, part):
    tile_order, lengths = order_and_lengths(key)
    starts = (jnp.cumsum(lengths) - lengths).astype(jnp.int32)
    tile_ids = jnp.arange(TILES).astype(jnp.int32)
    block_new = (jnp.sum((starts[None, :] <= tile_ids[:, None]).astype(jnp.int32), axis=1) - 1).astype(jnp.int32)
    block_old = jnp.zeros((TILES,), jnp.int32).at[tile_order].set(block_new)
    row_block = jnp.repeat(block_old, TILE)
    width = MOSTT * TILE
    factor_rows = jax.random.normal(jax.random.fold_in(key, 41), (ORDER, width), jnp.float32)
    gram = jnp.dot(factor_rows, factor_rows.T, precision=lax.Precision.HIGHEST) / width
    matrix = jnp.where(row_block[:, None] == row_block[None, :], gram, 0.0)
    noise_part = jax.random.normal(jax.random.fold_in(key, 47), (ORDER, ORDER), jnp.float32) * (0.08 / math.sqrt(2.0 * ORDER))
    matrix = matrix + noise_part
    matrix = matrix + noise_part.T
    diagonal = jax.random.uniform(jax.random.fold_in(key, 53), (ORDER,), jnp.float32, 0.4, 1.2)
    indices = jnp.arange(ORDER)
    return matrix.at[indices, indices].add(diagonal)


def shard_levels(rng, dims, shards, low, top_value):
    def one(dim, shards_of):
        heights = jax.random.uniform(jax.random.fold_in(jax.random.fold_in(rng, 6), dim), (shards_of,), jnp.float32, low / len(shards), top_value / len(shards))
        return jnp.repeat(jnp.exp(heights), dims[dim] // shards_of).reshape((-1,) + (1,) * (len(dims) - dim - 1))

    loudness = one(*shards[0])
    for cut in shards[1:]:
        loudness = loudness * one(*cut)
    return loudness


def centred(rng, dims, scale, most, pieces=(), kind=jnp.bfloat16):
    result = jax.random.normal(rng, dims, jnp.float32) * scale
    if len(pieces) > 0:
        result = shard_levels(rng, dims, pieces, -0.22, 0.18) * result
    return jnp.clip(result, min=-most, max=most).astype(kind)


def setup_inputs(seed: int = 0) -> dict:
    key_list = jax.random.split(jax.random.key(seed), 6)
    return {
        "normal_matrix": draw_normal_matrix(jax.random.fold_in(key_list[5], 71), 0),
        "right_sides": centred(key_list[1], (ORDER, RHS), 1.0, 6.0, ((0, 32),), jnp.float32),
        "tile_order": draw_tile_order(jax.random.fold_in(key_list[5], 71), 0),
        "inner_order": jax.vmap(lambda own: jax.random.permutation(own, TILE))(jax.random.split(key_list[3], TILES)).reshape((TILES, TILE)).astype(jnp.int32),
        "block_lengths": draw_block_lengths(jax.random.fold_in(key_list[5], 71), 0),
    }


def reference(normal_matrix, right_sides, tile_order, inner_order, block_lengths):
    window_rows = MOSTT * TILE
    new_to_old = (tile_order[:, None] * TILE + inner_order).reshape(-1).astype(jnp.int32)
    renumbered = jnp.take(jnp.take(normal_matrix, new_to_old, axis=0), new_to_old, axis=1)
    sides_ordered = jnp.take(right_sides, new_to_old, axis=0)
    lengths = block_lengths.astype(jnp.int32)
    starts = (jnp.cumsum(lengths) - lengths).astype(jnp.int32)
    tile_number = (jnp.arange(window_rows) // TILE).astype(jnp.int32)
    identity = jnp.eye(window_rows, dtype=jnp.float32)

    def corner_of(first_tile):
        window_tile = jnp.minimum(first_tile, TILES - MOSTT).astype(jnp.int32)
        shift_rows = ((first_tile - window_tile) * TILE).astype(jnp.int32)
        return ((window_tile * TILE).astype(jnp.int32), shift_rows)

    def factor_block(inputs):
        first_tile, length = inputs
        corner, shift_rows = corner_of(first_tile)
        block_matrix = lax.dynamic_slice(renumbered, (corner, corner), (window_rows, window_rows))
        block_matrix = jnp.roll(jnp.roll(block_matrix, -shift_rows, axis=0), -shift_rows, axis=1)
        inside = tile_number < length
        block_matrix = jnp.where(inside[:, None] & inside[None, :], block_matrix, identity)
        return jnp.linalg.cholesky(block_matrix)
    factors = lax.map(factor_block, (starts, lengths))
    tile_ids = jnp.arange(TILES).astype(jnp.int32)
    tile_block = (jnp.sum((starts[None, :] <= tile_ids[:, None]).astype(jnp.int32), axis=1) - 1).astype(jnp.int32)
    tile_position = (tile_ids - starts[tile_block]).astype(jnp.int32)

    def precondition(residual):

        def solve_block(inputs):
            factor, first_tile, length = inputs
            corner, shift_rows = corner_of(first_tile)
            segment = lax.dynamic_slice_in_dim(residual, corner, window_rows, 0)
            segment = jnp.roll(segment, -shift_rows, axis=0)
            segment = jnp.where((tile_number < length)[:, None], segment, 0.0)
            return jax.scipy.linalg.cho_solve((factor, True), segment)
        solved = lax.map(solve_block, (factors, starts, lengths))
        grouped = solved.reshape(starts.shape[0], MOSTT, TILE, residual.shape[1])
        return grouped[tile_block, tile_position].reshape(ORDER, residual.shape[1])
    iterate = precondition(sides_ordered)
    for sweep in range(ITERS):
        product_of = jnp.dot(renumbered.astype(jnp.float32), iterate.astype(jnp.float32), precision=lax.Precision.HIGHEST, preferred_element_type=jnp.float32)
        iterate = iterate + precondition(sides_ordered - product_of)
    return (renumbered, iterate)
```

```python
import jax
import jax.numpy as jnp
from jax import lax
from jax.experimental import pallas as pl
from jax.experimental.pallas import tpu as pltpu
from jax.sharding import PartitionSpec as P

MOSTT = 3
AXES = ("gx", "gy")
SUB = 8
HIGHEST = lax.Precision.HIGHEST


def dot(a, b, contract=((1,), (0,))):
    return lax.dot_general(
        a, b, (contract, ((), ())), precision=HIGHEST, preferred_element_type=jnp.float32
    )


def dot_t(a, b):
    return dot(a, b, ((1,), (1,)))


def one_pass(a, b):
    return lax.dot_general(a, b, (((1,), (0,)), ((), ())), preferred_element_type=jnp.float32)


def place_of_tile(order_ref, tiles, old_tile):
    def step(t, found):
        return jnp.where(order_ref[t] == old_tile, t, found)

    return lax.fori_loop(0, tiles, step, jnp.int32(0))


def block_of(lengths_ref, place):
    def step(e, carry):
        start, first, length = carry
        here = (start <= place) & (place < start + lengths_ref[e])
        first = jnp.where(here, start, first)
        length = jnp.where(here, lengths_ref[e], length)
        return start + lengths_ref[e], first, length

    zero = jnp.int32(0)
    _, first, length = lax.fori_loop(0, lengths_ref.shape[0], step, (zero, zero, zero + 1))
    return first, length


def pack_body(self_ref, order_ref, lengths_ref, inner_ref, slab_ref, sides_ref, send_ref, small_ref, rows_ref):
    tile = slab_ref.shape[0]
    tiles = order_ref.shape[0]
    rhs = sides_ref.shape[1]
    place = place_of_tile(order_ref, tiles, self_ref[0])
    first, length = block_of(lengths_ref, place)
    position = place - first
    own_inner = inner_ref[pl.ds(place, 1), :]
    hot = jnp.where(
        lax.broadcasted_iota(jnp.int32, (tile, tile), 0) == own_inner, 1.0, 0.0
    )
    row_hot = hot.T.astype(jnp.bfloat16)
    width = slab_ref.shape[1]
    step = min(width, 8 * tile)

    def order_rows(c, _):
        at = pl.ds(pl.multiple_of(c * step, step), step)
        x = slab_ref[:, at]
        high = x.astype(jnp.bfloat16)
        rest = x - high.astype(jnp.float32)
        middle = rest.astype(jnp.bfloat16)
        low = (rest - middle.astype(jnp.float32)).astype(jnp.bfloat16)
        rows_ref[:, at] = (one_pass(row_hot, low) + one_pass(row_hot, middle)) + one_pass(row_hot, high)
        return 0

    lax.fori_loop(0, width // step, order_rows, 0)

    def order_columns(t, _):
        at = pl.ds(pl.multiple_of(order_ref[t] * tile, tile), tile)
        chosen = jnp.broadcast_to(inner_ref[pl.ds(t, 1), :], (SUB, tile))
        for g in range(tile // SUB):
            x = rows_ref[g * SUB : (g + 1) * SUB, at]
            send_ref[t, g * SUB : (g + 1) * SUB, :] = jnp.take_along_axis(x, chosen, axis=1)
        return 0

    lax.fori_loop(0, tiles, order_columns, 0)

    after = jnp.where(position == MOSTT - 1, 0, position + 1)
    beside = jnp.minimum(first + after, tiles - 1)
    turned = sides_ref[...].T
    sides_turned = jnp.take_along_axis(turned, jnp.broadcast_to(own_inner, (rhs, tile)), axis=1)
    pieces = 2 * tile // SUB
    per_piece = rhs // pieces
    for k in range(pieces):
        if k < pieces // 2:
            chunk = send_ref[place, k * SUB : (k + 1) * SUB, :]
        else:
            at = (k - pieces // 2) * SUB
            chunk = send_ref[beside, at : at + SUB, :]
        small_ref[k, 0:SUB, :] = chunk
        small_ref[k, SUB : 2 * SUB, :] = jnp.zeros((SUB, tile), jnp.float32)
        small_ref[k, SUB : SUB + per_piece, :] = sides_turned[k * per_piece : (k + 1) * per_piece, :]
    for k in range(pieces, tiles):
        small_ref[k] = jnp.zeros(small_ref.shape[1:], jnp.float32)


def route_body(order_ref, lengths_ref, got_ref, send_ref, first_ref, *, per_piece):
    tiles = order_ref.shape[0]

    def block(e, start):
        for j in range(MOSTT):
            @pl.when(j < lengths_ref[e])
            def _():
                first_ref[start + j] = start
        return start + lengths_ref[e]

    lax.fori_loop(0, lengths_ref.shape[0], block, jnp.int32(0))
    spare = send_ref.shape[1] - MOSTT * SUB

    def fill(d, _):
        send_ref[d, MOSTT * SUB :, :] = jnp.zeros((spare, send_ref.shape[2]), jnp.float32)
        for m in range(MOSTT):
            source = order_ref[jnp.minimum(first_ref[d] + m, tiles - 1)]
            send_ref[d, m * SUB : (m + 1) * SUB, :] = got_ref[source, 0:SUB, :]
            at = MOSTT * SUB + m * per_piece
            send_ref[d, at : at + per_piece, :] = got_ref[source, SUB : SUB + per_piece, :]
        return 0

    lax.fori_loop(0, tiles, fill, 0)


def sweep(s):
    for k in range(SUB):
        inverse = pltpu.reciprocal(s[k][k], approx=False)
        column = [s[max(i, k)][min(i, k)] for i in range(SUB)]
        scaled = [column[i] * inverse for i in range(SUB)]
        for i in range(SUB):
            for j in range(i + 1):
                if i != k and j != k:
                    s[i][j] = s[i][j] - scaled[i] * column[j]
        for i in range(SUB):
            if i != k:
                s[max(i, k)][min(i, k)] = scaled[i]
        s[k][k] = -inverse
    return s


def invert_in_place(m_ref):
    size = m_ref.shape[0]
    lane = lax.broadcasted_iota(jnp.int32, (SUB, size), 1)
    sub = lax.broadcasted_iota(jnp.int32, (SUB, size), 0)

    def panel(p, _):
        row = pl.multiple_of(p * SUB, SUB)
        rows = m_ref[pl.ds(row, SUB), :]
        inside = (lane >= row) & (lane < row + SUB)
        at = [jnp.full((SUB, size), row + j, jnp.int32) for j in range(SUB)]
        columns = [jnp.take_along_axis(rows, at[j], axis=1) for j in range(SUB)]
        s = [
            [jnp.broadcast_to(columns[j][i : i + 1, :], (SUB, size)) for j in range(i + 1)]
            for i in range(SUB)
        ]
        s = sweep(s)
        spread = [
            jnp.where(
                inside,
                jnp.where(lane == row + j, 1.0, 0.0),
                jnp.broadcast_to(rows[j : j + 1, :], (SUB, size)),
            )
            for j in range(SUB)
        ]
        update = []
        for i in range(SUB):
            total = s[i][0] * spread[0]
            for j in range(1, SUB):
                total = total + s[max(i, j)][min(i, j)] * spread[j]
            update.append(total)
        new = -update[0]
        for i in range(1, SUB):
            new = jnp.where(sub == i, -update[i], new)
        for g in range(size // SUB):
            here = m_ref[g * SUB : (g + 1) * SUB, :]
            total = jnp.where(inside, 0.0, here)
            for j in range(SUB):
                total = total + jnp.take_along_axis(here, at[j], axis=1) * update[j]
            m_ref[g * SUB : (g + 1) * SUB, :] = total
        m_ref[pl.ds(row, SUB), :] = new
        return 0

    lax.fori_loop(0, size // SUB, panel, 0)


def apply_inverse(f_ref, b):
    y1 = b[1] - dot(b[0], f_ref[3])
    y2 = b[2] - dot(b[0], f_ref[4]) - dot(y1, f_ref[5])
    z2 = dot(y2, f_ref[2])
    z1 = dot(y1, f_ref[1]) - dot_t(z2, f_ref[5])
    z0 = dot(b[0], f_ref[0]) - dot_t(z1, f_ref[3]) - dot_t(z2, f_ref[4])
    return z0, z1, z2


def pick(position, values):
    chosen = values[0]
    for m in range(1, len(values)):
        chosen = jnp.where(position == m, values[m], chosen)
    return chosen


def factor_body(self_ref, lengths_ref, got_ref, f_ref, b_ref, z_ref, zs_ref, o_ref, bs_ref, *, per_piece):
    tile = got_ref.shape[2]
    pieces = 2 * tile // SUB
    place = self_ref[0]
    first, length = block_of(lengths_ref, place)
    position = place - first
    eye = jnp.where(
        lax.broadcasted_iota(jnp.int32, (SUB, tile), 0)
        == lax.broadcasted_iota(jnp.int32, (SUB, tile), 1),
        1.0,
        0.0,
    )
    lane = lax.broadcasted_iota(jnp.int32, (SUB, tile), 1)
    sub = lax.broadcasted_iota(jnp.int32, (SUB, tile), 0)
    for m in range(MOSTT):
        pair_inside = m + 1 < length if m < MOSTT - 1 else m < length
        for k in range(pieces // 2):
            diagonal = jnp.where(lane == sub + k * SUB, 1.0, 0.0)
            at = slice(k * SUB, (k + 1) * SUB)
            f_ref[m, at, :] = jnp.where(m < length, got_ref[k, m * SUB : (m + 1) * SUB, :], diagonal)
            beside = got_ref[k + pieces // 2, m * SUB : (m + 1) * SUB, :]
            o_ref[m, at, :] = jnp.where(pair_inside, beside, 0.0)
        for k in range(pieces):
            start = MOSTT * SUB + m * per_piece
            part = got_ref[k, start : start + per_piece, :]
            bs_ref[m, k * per_piece : (k + 1) * per_piece, :] = jnp.where(m < length, part, 0.0)
    a01 = o_ref[0]
    a12 = o_ref[1]
    a20 = o_ref[2]
    a10 = a01.T
    invert_in_place(f_ref.at[0])
    w01 = dot(f_ref[0], a01)
    w02 = dot_t(f_ref[0], a20)
    f_ref[3] = w01
    f_ref[4] = w02
    f_ref[1] = f_ref[1] - dot(a10, w01)
    s12 = a12 - dot(a10, w02)
    invert_in_place(f_ref.at[1])
    w12 = dot(f_ref[1], s12)
    f_ref[5] = w12
    f_ref[2] = f_ref[2] - dot(a20, w02) - dot(s12.T, w12)
    invert_in_place(f_ref.at[2])
    b = [bs_ref[m] for m in range(MOSTT)]
    z = pick(position, apply_inverse(f_ref, b))
    b_ref[...] = pick(position, b)
    z_ref[...] = z
    for d in range(zs_ref.shape[0]):
        zs_ref[d] = z


def arrange_body(order_ref, got_ref, slab_ref):
    tiles = order_ref.shape[0]
    tile = got_ref.shape[1]

    def move(t, _):
        slab_ref[pl.ds(pl.multiple_of(t * tile, tile), tile), :] = got_ref[order_ref[t]]
        return 0

    lax.fori_loop(0, tiles, move, 0)


def residual_body(slab_ref, iterate_ref, b_ref, r_ref):
    tiles, rhs, tile = iterate_ref.shape
    group = 8
    total = b_ref[...]
    for c in range(tiles // group):
        x = jnp.concatenate([iterate_ref[c * group + t] for t in range(group)], axis=1)
        total = total - dot(x, slab_ref[c * group * tile : (c + 1) * group * tile, :])
    r_ref[...] = total


def finish_body(self_ref, lengths_ref, f_ref, z_ref, *rest):
    near_refs, out_ref, all_ref = rest[:-2], rest[-2], rest[-1]
    place = self_ref[0]
    first, length = block_of(lengths_ref, place)
    position = place - first
    for i, near_ref in enumerate(near_refs):
        all_ref[i] = near_ref[...]
    b = []
    for m in range(MOSTT):
        r = all_ref[jnp.clip(MOSTT - 1 + m - position, 0, len(near_refs) - 1)]
        b.append(jnp.where(m < length, r, 0.0))
    total = z_ref[...] + pick(position, apply_inverse(f_ref, b))
    out_ref[...] = total.T


def shift(value, steps):
    count = lax.axis_size(AXES)
    pairs = [(s, s + steps) for s in range(count) if 0 <= s + steps < count]
    return lax.ppermute(value, AXES, pairs)


def exchange(value):
    n, rows, lanes = value.shape
    moved = lax.all_to_all(value.reshape(n * rows, lanes), AXES, 0, 0, tiled=True)
    return moved.reshape(n, rows, lanes)


def body(normal_matrix, right_sides, tile_order, inner_order, block_lengths):
    f32 = jnp.float32
    tile = normal_matrix.shape[0]
    rhs = right_sides.shape[1]
    tiles = tile_order.shape[0]
    per_piece = rhs // (2 * tile // SUB)
    me = lax.axis_index(AXES).astype(jnp.int32).reshape(1)
    smem = pl.BlockSpec(memory_space=pltpu.SMEM)
    vmem = pl.BlockSpec(memory_space=pltpu.VMEM)
    shape = lambda *dims: jax.ShapeDtypeStruct(dims, f32)

    tiles_out, small = pl.pallas_call(
        pack_body,
        out_shape=(shape(tiles, tile, tile), shape(tiles, 2 * SUB, tile)),
        in_specs=[smem, smem, smem, vmem, vmem, vmem],
        out_specs=(vmem, vmem),
        scratch_shapes=[pltpu.VMEM(normal_matrix.shape, f32)],
        name="pack",
    )(me, tile_order, block_lengths, inner_order, normal_matrix, right_sides)

    small_got = exchange(small)
    routed_rows = MOSTT * SUB + -(-MOSTT * per_piece // SUB) * SUB
    routed = pl.pallas_call(
        lambda *refs: route_body(*refs, per_piece=per_piece),
        out_shape=shape(tiles, routed_rows, tile),
        in_specs=[smem, smem, vmem],
        out_specs=vmem,
        scratch_shapes=[pltpu.SMEM((tiles,), jnp.int32)],
        name="route",
    )(tile_order, block_lengths, small_got)
    block_parts = exchange(routed)
    tiles_got = exchange(tiles_out)

    factors, own_sides, z, z_spread = pl.pallas_call(
        lambda *refs: factor_body(*refs, per_piece=per_piece),
        out_shape=(
            shape(2 * MOSTT, tile, tile),
            shape(rhs, tile),
            shape(rhs, tile),
            shape(tiles, rhs, tile),
        ),
        in_specs=[smem, smem, vmem],
        out_specs=(vmem, vmem, vmem, vmem),
        scratch_shapes=[
            pltpu.VMEM((MOSTT, tile, tile), f32),
            pltpu.VMEM((MOSTT, rhs, tile), f32),
        ],
        name="factor",
    )(me, block_lengths, block_parts)

    iterate = exchange(z_spread)
    slab = pl.pallas_call(
        arrange_body,
        out_shape=shape(tiles * tile, tile),
        in_specs=[smem, vmem],
        out_specs=vmem,
        name="arrange",
    )(tile_order, tiles_got)
    residual = pl.pallas_call(
        residual_body,
        out_shape=shape(rhs, tile),
        in_specs=[vmem, vmem, vmem],
        out_specs=vmem,
        name="residual",
    )(slab, iterate, own_sides)
    near = [
        residual if o == 0 else shift(residual, -o) for o in range(1 - MOSTT, MOSTT)
    ]
    solved = pl.pallas_call(
        finish_body,
        out_shape=shape(tile, rhs),
        in_specs=[smem, smem, vmem, vmem] + [vmem] * len(near),
        out_specs=vmem,
        scratch_shapes=[pltpu.VMEM((len(near), rhs, tile), f32)],
        name="finish",
    )(me, block_lengths, factors, z, *near)
    return slab, solved


def solution(mesh):
    placed = (P(AXES, None), P(AXES, None), P(), P(), P())
    return jax.shard_map(
        body,
        mesh=mesh,
        in_specs=placed,
        out_specs=(P(None, AXES), P(AXES, None)),
        check_vma=False,
    )
```

```python
import jax
import jax.numpy as jnp
from jax import lax
from jax.experimental import pallas as pl
from jax.experimental.pallas import tpu as pltpu
from jax.sharding import PartitionSpec as P


MOSTT = 3
AXES = ("gx", "gy")
SUB = 8
HIGHEST = lax.Precision.HIGHEST


def dot(a, b, contract=((1,), (0,))):
    return lax.dot_general(
        a, b, (contract, ((), ())), precision=HIGHEST, preferred_element_type=jnp.float32
    )


def dot_t(a, b):
    return dot(a, b, ((1,), (1,)))


def one_pass(a, b):
    return lax.dot_general(a, b, (((1,), (0,)), ((), ())), preferred_element_type=jnp.float32)


def place_of_tile(order_ref, tiles, old_tile):
    def step(t, found):
        return jnp.where(order_ref[t] == old_tile, t, found)

    return lax.fori_loop(0, tiles, step, jnp.int32(0))


def block_of(lengths_ref, place):
    def step(e, carry):
        start, first, length = carry
        here = (start <= place) & (place < start + lengths_ref[e])
        first = jnp.where(here, start, first)
        length = jnp.where(here, lengths_ref[e], length)
        return start + lengths_ref[e], first, length

    zero = jnp.int32(0)
    _, first, length = lax.fori_loop(0, lengths_ref.shape[0], step, (zero, zero, zero + 1))
    return first, length


def split_rows(hot, x):
    high = x.astype(jnp.bfloat16)
    rest = x - high.astype(jnp.float32)
    middle = rest.astype(jnp.bfloat16)
    low = (rest - middle.astype(jnp.float32)).astype(jnp.bfloat16)
    return (one_pass(hot, low) + one_pass(hot, middle)) + one_pass(hot, high)


def row_choice(inner_row, tile):
    hot = jnp.where(lax.broadcasted_iota(jnp.int32, (tile, tile), 0) == inner_row, 1.0, 0.0)
    return hot.T.astype(jnp.bfloat16)


def sides_fit(tile, rhs):
    return 4 * rhs == tile


def near_body(self_ref, order_ref, lengths_ref, inner_ref, sides_ref, slab_ref, small_ref, near_ref, sems):
    tile = slab_ref.shape[0]
    tiles = order_ref.shape[0]
    rhs = sides_ref.shape[0]
    me = self_ref[0]
    place = place_of_tile(order_ref, tiles, me)
    first, _ = block_of(lengths_ref, place)
    position = place - first
    after = jnp.where(position == MOSTT - 1, 0, position + 1)
    beside = jnp.minimum(first + after, tiles - 1)
    places = (place, beside)
    copies = []
    for i, t in enumerate(places):
        at = pl.ds(pl.multiple_of(order_ref[t] * tile, tile), tile)
        copies.append(pltpu.make_async_copy(slab_ref.at[:, at], near_ref.at[i], sems.at[i]))
        copies[-1].start()
    own_inner = inner_ref[pl.ds(place, 1), :]
    row_hot = row_choice(own_inner, tile)
    turned = jnp.take_along_axis(
        sides_ref[...], jnp.broadcast_to(own_inner, (rhs, tile)), axis=1
    )
    pieces = 2 * tile // SUB
    rows = small_ref.shape[0] // tiles
    half = tile // 2
    lane = lax.broadcasted_iota(jnp.int32, (SUB, tile), 1)
    if small_ref.shape[0] > pieces * rows:
        small_ref[pieces * rows :, :] = jnp.zeros((small_ref.shape[0] - pieces * rows, tile), jnp.float32)
    for i, t in enumerate(places):
        copies[i].wait()
        moved = split_rows(row_hot, near_ref[i])
        chosen = jnp.broadcast_to(inner_ref[pl.ds(t, 1), :], (tile, tile))
        moved = jnp.take_along_axis(moved, chosen, axis=1)
        if i == 0 and sides_fit(tile, rhs):
            extra = jnp.concatenate([turned, pltpu.roll(turned, half, 1)], axis=0)
        for k in range(pieces // 2):
            chunk = moved[k * SUB : (k + 1) * SUB, :]
            if i == 0 and sides_fit(tile, rhs) and k * SUB >= half:
                chunk = jnp.where(lane < half, extra[k * SUB - half : (k + 1) * SUB - half, :], chunk)
            at = (i * (pieces // 2) + k) * rows
            small_ref[at : at + SUB, :] = chunk
    if not sides_fit(tile, rhs):
        per_piece = rhs // pieces
        for k in range(pieces):
            at = k * rows + SUB
            small_ref[at : at + SUB, :] = jnp.zeros((SUB, tile), jnp.float32)
            small_ref[at : at + per_piece, :] = turned[k * per_piece : (k + 1) * per_piece, :]


def pack_body(self_ref, order_ref, inner_ref, slab_ref, send_ref, rows_ref):
    tile = slab_ref.shape[0]
    tiles = order_ref.shape[0]
    place = place_of_tile(order_ref, tiles, self_ref[0])
    row_hot = row_choice(inner_ref[pl.ds(place, 1), :], tile)
    width = slab_ref.shape[1]
    step = min(width, 8 * tile)

    def order_rows(c, _):
        at = pl.ds(pl.multiple_of(c * step, step), step)
        rows_ref[:, at] = split_rows(row_hot, slab_ref[:, at])
        return 0

    lax.fori_loop(0, width // step, order_rows, 0)

    def order_columns(t, _):
        at = pl.ds(pl.multiple_of(order_ref[t] * tile, tile), tile)
        chosen = jnp.broadcast_to(inner_ref[pl.ds(t, 1), :], (SUB, tile))
        for g in range(tile // SUB):
            x = rows_ref[g * SUB : (g + 1) * SUB, at]
            send_ref[t, g * SUB : (g + 1) * SUB, :] = jnp.take_along_axis(x, chosen, axis=1)
        return 0

    lax.fori_loop(0, tiles, order_columns, 0)


def route_body(order_ref, lengths_ref, got_ref, send_ref, first_ref, *, per_piece):
    tiles = order_ref.shape[0]

    def block(e, start):
        for j in range(MOSTT):
            @pl.when(j < lengths_ref[e])
            def _():
                first_ref[start + j] = start
        return start + lengths_ref[e]

    lax.fori_loop(0, lengths_ref.shape[0], block, jnp.int32(0))
    spare = send_ref.shape[1] - MOSTT * SUB

    def fill(d, _):
        if spare:
            send_ref[d, MOSTT * SUB :, :] = jnp.zeros((spare, send_ref.shape[2]), jnp.float32)
        for m in range(MOSTT):
            source = order_ref[jnp.minimum(first_ref[d] + m, tiles - 1)]
            send_ref[d, m * SUB : (m + 1) * SUB, :] = got_ref[source, 0:SUB, :]
            if spare:
                at = MOSTT * SUB + m * per_piece
                send_ref[d, at : at + per_piece, :] = got_ref[source, SUB : SUB + per_piece, :]
        return 0

    lax.fori_loop(0, tiles, fill, 0)


def sweep(s):
    for k in range(SUB):
        inverse = pltpu.reciprocal(s[k][k], approx=False)
        column = [s[max(i, k)][min(i, k)] for i in range(SUB)]
        scaled = [column[i] * inverse for i in range(SUB)]
        for i in range(SUB):
            for j in range(i + 1):
                if i != k and j != k:
                    s[i][j] = s[i][j] - scaled[i] * column[j]
        for i in range(SUB):
            if i != k:
                s[max(i, k)][min(i, k)] = scaled[i]
        s[k][k] = -inverse
    return s


def invert_in_place(m_ref):
    size = m_ref.shape[0]
    lane = lax.broadcasted_iota(jnp.int32, (SUB, size), 1)
    sub = lax.broadcasted_iota(jnp.int32, (SUB, size), 0)

    def panel(p, _):
        row = pl.multiple_of(p * SUB, SUB)
        rows = m_ref[pl.ds(row, SUB), :]
        inside = (lane >= row) & (lane < row + SUB)
        at = [jnp.full((SUB, size), row + j, jnp.int32) for j in range(SUB)]
        columns = [jnp.take_along_axis(rows, at[j], axis=1) for j in range(SUB)]
        s = [
            [jnp.broadcast_to(columns[j][i : i + 1, :], (SUB, size)) for j in range(i + 1)]
            for i in range(SUB)
        ]
        s = sweep(s)
        spread = [
            jnp.where(
                inside,
                jnp.where(lane == row + j, 1.0, 0.0),
                jnp.broadcast_to(rows[j : j + 1, :], (SUB, size)),
            )
            for j in range(SUB)
        ]
        update = []
        for i in range(SUB):
            total = s[i][0] * spread[0]
            for j in range(1, SUB):
                total = total + s[max(i, j)][min(i, j)] * spread[j]
            update.append(total)
        new = -update[0]
        for i in range(1, SUB):
            new = jnp.where(sub == i, -update[i], new)
        for g in range(size // SUB):
            here = m_ref[g * SUB : (g + 1) * SUB, :]
            total = jnp.where(inside, 0.0, here)
            for j in range(SUB):
                total = total + jnp.take_along_axis(here, at[j], axis=1) * update[j]
            m_ref[g * SUB : (g + 1) * SUB, :] = total
        m_ref[pl.ds(row, SUB), :] = new
        return 0

    lax.fori_loop(0, size // SUB, panel, 0)


def block_inverse(f_ref, w01, w02, w12):
    e0, e1, e2 = f_ref[0], f_ref[1], f_ref[2]
    v12 = -dot(w12, e2)
    v11 = e1 - dot_t(v12, w12)
    v02 = -dot(w01, v12) - dot(w02, e2)
    v01 = -dot(w01, v11) - dot_t(w02, v12)
    v00 = e0 - dot_t(v01, w01) - dot_t(v02, w02)
    return (v00, v01, v02), (v01.T, v11, v12), (v02.T, v12.T, e2)


def apply_rows(v_ref, b):
    return dot_t(jnp.concatenate(b, axis=1), v_ref[...])


def pick(position, values):
    chosen = values[0]
    for m in range(1, len(values)):
        chosen = jnp.where(position == m, values[m], chosen)
    return chosen


def factor_body(self_ref, lengths_ref, got_ref, v_ref, b_ref, z_ref, f_ref, o_ref, bs_ref, *, per_piece):
    tile = got_ref.shape[2]
    rhs = b_ref.shape[0]
    pieces = 2 * tile // SUB
    half = tile // 2
    first, length = block_of(lengths_ref, self_ref[0])
    position = self_ref[0] - first
    row = lax.broadcasted_iota(jnp.int32, (tile, tile), 0)
    lane = lax.broadcasted_iota(jnp.int32, (tile, tile), 1)
    for m in range(MOSTT):
        pair_inside = m + 1 < length if m < MOSTT - 1 else m < length
        for k in range(pieces // 2):
            at = slice(k * SUB, (k + 1) * SUB)
            f_ref[m, at, :] = got_ref[k, m * SUB : (m + 1) * SUB, :]
            beside = got_ref[k + pieces // 2, m * SUB : (m + 1) * SUB, :]
            o_ref[m, at, :] = jnp.where(pair_inside, beside, 0.0)
        own = f_ref[m]
        if sides_fit(tile, rhs):
            low = own[half : half + rhs, :]
            high = pltpu.roll(own[half + rhs :, :], half, 1)
            side = jnp.where(lane[:rhs, :] < half, low, high)
            own = jnp.where((row >= half) & (lane < half), own.T, own)
            bs_ref[m] = jnp.where(m < length, side, 0.0)
        else:
            for k in range(pieces):
                start = MOSTT * SUB + m * per_piece
                part = got_ref[k, start : start + per_piece, :]
                bs_ref[m, k * per_piece : (k + 1) * per_piece, :] = jnp.where(m < length, part, 0.0)
        f_ref[m] = jnp.where(m < length, own, jnp.where(row == lane, 1.0, 0.0))
    a01 = o_ref[0]
    a12 = o_ref[1]
    a20 = o_ref[2]
    a10 = a01.T
    invert_in_place(f_ref.at[0])
    w01 = dot(f_ref[0], a01)
    w02 = dot_t(f_ref[0], a20)
    f_ref[1] = f_ref[1] - dot(a10, w01)
    s12 = a12 - dot(a10, w02)
    invert_in_place(f_ref.at[1])
    w12 = dot(f_ref[1], s12)
    f_ref[2] = f_ref[2] - dot(a20, w02) - dot(s12.T, w12)
    invert_in_place(f_ref.at[2])
    rows = block_inverse(f_ref, w01, w02, w12)
    for m in range(MOSTT):
        v_ref[:, m * tile : (m + 1) * tile] = pick(position, [rows[p][m] for p in range(MOSTT)])
    b = [bs_ref[m] for m in range(MOSTT)]
    b_ref[...] = pick(position, b)
    z_ref[...] = apply_rows(v_ref, b)


def arrange_body(order_ref, got_ref, slab_ref):
    tiles = order_ref.shape[0]
    tile = got_ref.shape[1]

    def move(t, _):
        slab_ref[pl.ds(pl.multiple_of(t * tile, tile), tile), :] = got_ref[order_ref[t]]
        return 0

    lax.fori_loop(0, tiles, move, 0)


def residual_body(self_ref, order_ref, got_ref, b_ref, *rest, flips):
    part_refs, r_ref, x_ref = rest[:-2], rest[-2], rest[-1]
    _, tile = b_ref.shape
    tiles = order_ref.shape[0]
    me = self_ref[0]
    j = 0
    for part_ref in part_refs:
        for i in range(part_ref.shape[0]):
            at = pl.multiple_of(order_ref[me ^ flips[j]] * tile, tile)
            x_ref[:, pl.ds(at, tile)] = part_ref[i]
            j += 1
    group = 8
    total = b_ref[...]
    for c in range(tiles // group):
        x = x_ref[:, c * group * tile : (c + 1) * group * tile]
        g = got_ref[c * group : (c + 1) * group].reshape(group * tile, tile)
        total = total - dot(x, g)
    r_ref[...] = total


def finish_body(self_ref, lengths_ref, v_ref, z_ref, *rest):
    near_refs, out_ref, all_ref = rest[:-2], rest[-2], rest[-1]
    place = self_ref[0]
    first, length = block_of(lengths_ref, place)
    position = place - first
    for i, near_ref in enumerate(near_refs):
        all_ref[i] = near_ref[...]
    b = []
    for m in range(MOSTT):
        r = all_ref[jnp.clip(MOSTT - 1 + m - position, 0, len(near_refs) - 1)]
        b.append(jnp.where(m < length, r, 0.0))
    out_ref[...] = z_ref[...] + apply_rows(v_ref, b)


def shift(value, steps):
    count = lax.axis_size(AXES)
    return lax.ppermute(value, AXES, [(s, (s + steps) % count) for s in range(count)])


def exchange(value, rows):
    lanes = value.shape[-1]
    moved = lax.all_to_all(value.reshape(-1, lanes), AXES, 0, 0, tiled=True)
    return moved.reshape(-1, rows, lanes)


def swap(value, bit):
    count = lax.axis_size(AXES)
    return lax.ppermute(value, AXES, [(s, s ^ bit) for s in range(count)])


def spread(value):
    count_x, count_y = lax.axis_size("gx"), lax.axis_size("gy")
    assert count_x & (count_x - 1) == 0 and count_y & (count_y - 1) == 0
    low = 1 << ((count_y.bit_length() - 1) // 2)
    held, flips = value[None], [0]
    bits = [count_y << i for i in range(1, count_x.bit_length() - 1)]
    bits += [1 << i for i in range(low.bit_length() - 1)]
    for bit in bits:
        held = jnp.concatenate([held, swap(held, bit)], axis=0)
        flips += [f ^ bit for f in flips]
    across = [low * i for i in range(1, count_y // low)]
    parts = [held] + [swap(held, bit) for bit in across]
    held = jnp.concatenate(parts, axis=0)
    flips += [f ^ bit for bit in across for f in flips]
    if count_x > 1:
        parts = [held, swap(held, count_y)]
        flips += [f ^ count_y for f in flips]
    else:
        parts = [held]
    return parts, tuple(flips)


def body(normal_matrix, right_sides, tile_order, inner_order, block_lengths):
    f32 = jnp.float32
    tile = normal_matrix.shape[0]
    rhs = right_sides.shape[1]
    tiles = tile_order.shape[0]
    per_piece = rhs // (2 * tile // SUB)
    fit = sides_fit(tile, rhs)
    me = lax.axis_index(AXES).astype(jnp.int32).reshape(1)
    smem = pl.BlockSpec(memory_space=pltpu.SMEM)
    vmem = pl.BlockSpec(memory_space=pltpu.VMEM)
    hbm = pl.BlockSpec(memory_space=pl.ANY)
    shape = lambda *dims: jax.ShapeDtypeStruct(dims, f32)

    small_rows = SUB if fit else 2 * SUB
    small = pl.pallas_call(
        near_body,
        out_shape=shape(tiles * small_rows, tile),
        in_specs=[smem, smem, smem, vmem, vmem, hbm],
        out_specs=vmem,
        scratch_shapes=[pltpu.VMEM((2, tile, tile), f32), pltpu.SemaphoreType.DMA((2,))],
        name="near",
    )(me, tile_order, block_lengths, inner_order, right_sides.T, normal_matrix)
    small_got = exchange(small, small_rows)
    tiles_out = pl.pallas_call(
        pack_body,
        out_shape=shape(tiles, tile, tile),
        in_specs=[smem, smem, vmem, vmem],
        out_specs=vmem,
        scratch_shapes=[pltpu.VMEM(normal_matrix.shape, f32)],
        name="pack",
    )(me, tile_order, inner_order, normal_matrix)
    routed_rows = MOSTT * SUB + (0 if fit else -(-MOSTT * per_piece // SUB) * SUB)
    routed = pl.pallas_call(
        lambda *refs: route_body(*refs, per_piece=per_piece),
        out_shape=shape(tiles, routed_rows, tile),
        in_specs=[smem, smem, vmem],
        out_specs=vmem,
        scratch_shapes=[pltpu.SMEM((tiles,), jnp.int32)],
        name="route",
    )(tile_order, block_lengths, small_got)
    block_parts = exchange(routed, routed_rows)
    tiles_got = exchange(tiles_out, tile)

    inverse_rows, own_sides, z = pl.pallas_call(
        lambda *refs: factor_body(*refs, per_piece=per_piece),
        out_shape=(shape(tile, MOSTT * tile), shape(rhs, tile), shape(rhs, tile)),
        in_specs=[smem, smem, vmem],
        out_specs=(vmem, vmem, vmem),
        scratch_shapes=[
            pltpu.VMEM((MOSTT, tile, tile), f32),
            pltpu.VMEM((MOSTT, tile, tile), f32),
            pltpu.VMEM((MOSTT, rhs, tile), f32),
        ],
        name="factor",
    )(me, block_lengths, block_parts)

    iterate, flips = spread(z)
    slab = pl.pallas_call(
        arrange_body,
        out_shape=shape(tiles * tile, tile),
        in_specs=[smem, vmem],
        out_specs=vmem,
        name="arrange",
    )(tile_order, tiles_got)
    residual = pl.pallas_call(
        lambda *refs: residual_body(*refs, flips=flips),
        out_shape=shape(rhs, tile),
        in_specs=[smem, smem, vmem, vmem] + [vmem] * len(iterate),
        out_specs=vmem,
        scratch_shapes=[pltpu.VMEM((rhs, tiles * tile), f32)],
        name="residual",
    )(me, tile_order, tiles_got, own_sides, *iterate)
    near = [
        residual if o == 0 else shift(residual, -o) for o in range(1 - MOSTT, MOSTT)
    ]
    solved = pl.pallas_call(
        finish_body,
        out_shape=shape(rhs, tile),
        in_specs=[smem, smem, vmem, vmem] + [vmem] * len(near),
        out_specs=vmem,
        scratch_shapes=[pltpu.VMEM((len(near), rhs, tile), f32)],
        name="finish",
    )(me, block_lengths, inverse_rows, z, *near)
    return slab, solved.T


def solution(mesh):
    placed = (P(AXES, None), P(AXES, None), P(), P(), P())
    return jax.shard_map(
        body,
        mesh=mesh,
        in_specs=placed,
        out_specs=(P(None, AXES), P(AXES, None)),
        check_vma=False,
    )
```

```python
import math

import jax
import jax.numpy as jnp
from jax import lax
from jax.experimental import pallas as pl
from jax.experimental.pallas import tpu as pltpu
from jax.sharding import PartitionSpec as P


MOSTT = 3
AXES = ("gx", "gy")
SUB = 8
HIGHEST = lax.Precision.HIGHEST


def dot(a, b, contract=((1,), (0,))):
    return lax.dot_general(
        a, b, (contract, ((), ())), precision=HIGHEST, preferred_element_type=jnp.float32
    )


def dot_t(a, b):
    return dot(a, b, ((1,), (1,)))


def one_pass(a, b):
    return lax.dot_general(a, b, (((1,), (0,)), ((), ())), preferred_element_type=jnp.float32)


def place_of_tile(order_ref, tiles, old_tile):
    def step(t, found):
        return jnp.where(order_ref[t] == old_tile, t, found)

    return lax.fori_loop(0, tiles, step, jnp.int32(0), unroll=8)


def block_of(lengths_ref, place):
    def step(e, carry):
        start, first, length = carry
        here = (start <= place) & (place < start + lengths_ref[e])
        first = jnp.where(here, start, first)
        length = jnp.where(here, lengths_ref[e], length)
        return start + lengths_ref[e], first, length

    zero = jnp.int32(0)
    _, first, length = lax.fori_loop(
        0, lengths_ref.shape[0], step, (zero, zero, zero + 1), unroll=8
    )
    return first, length


def split_rows(hot, x):
    high = x.astype(jnp.bfloat16)
    rest = x - high.astype(jnp.float32)
    middle = rest.astype(jnp.bfloat16)
    low = (rest - middle.astype(jnp.float32)).astype(jnp.bfloat16)
    return (one_pass(hot, low) + one_pass(hot, middle)) + one_pass(hot, high)


def row_choice(inner_row, tile):
    hot = jnp.where(lax.broadcasted_iota(jnp.int32, (tile, tile), 0) == inner_row, 1.0, 0.0)
    return hot.T.astype(jnp.bfloat16)


def sides_fit(tile, rhs):
    return 4 * rhs == tile


def near_body(self_ref, order_ref, lengths_ref, inner_ref, sides_ref, slab_ref, small_ref, near_ref, sems):
    tile = slab_ref.shape[0]
    tiles = order_ref.shape[0]
    rhs = sides_ref.shape[0]
    me = self_ref[0]
    place = place_of_tile(order_ref, tiles, me)
    first, _ = block_of(lengths_ref, place)
    position = place - first
    after = jnp.where(position == MOSTT - 1, 0, position + 1)
    beside = jnp.minimum(first + after, tiles - 1)
    places = (place, beside)
    copies = []
    for i, t in enumerate(places):
        at = pl.ds(pl.multiple_of(order_ref[t] * tile, tile), tile)
        copies.append(pltpu.make_async_copy(slab_ref.at[:, at], near_ref.at[i], sems.at[i]))
        copies[-1].start()
    own_inner = inner_ref[pl.ds(place, 1), :]
    row_hot = row_choice(own_inner, tile)
    turned = jnp.take_along_axis(
        sides_ref[...], jnp.broadcast_to(own_inner, (rhs, tile)), axis=1
    )
    pieces = 2 * tile // SUB
    rows = small_ref.shape[0] // tiles
    half = tile // 2
    lane = lax.broadcasted_iota(jnp.int32, (SUB, tile), 1)
    if small_ref.shape[0] > pieces * rows:
        small_ref[pieces * rows :, :] = jnp.zeros((small_ref.shape[0] - pieces * rows, tile), jnp.float32)
    for i, t in enumerate(places):
        copies[i].wait()
        moved = split_rows(row_hot, near_ref[i])
        chosen = jnp.broadcast_to(inner_ref[pl.ds(t, 1), :], (tile, tile))
        moved = jnp.take_along_axis(moved, chosen, axis=1)
        if i == 0 and sides_fit(tile, rhs):
            extra = jnp.concatenate([turned, pltpu.roll(turned, half, 1)], axis=0)
        for k in range(pieces // 2):
            chunk = moved[k * SUB : (k + 1) * SUB, :]
            if i == 0 and sides_fit(tile, rhs) and k * SUB >= half:
                chunk = jnp.where(lane < half, extra[k * SUB - half : (k + 1) * SUB - half, :], chunk)
            at = (i * (pieces // 2) + k) * rows
            small_ref[at : at + SUB, :] = chunk
    if not sides_fit(tile, rhs):
        per_piece = rhs // pieces
        for k in range(pieces):
            at = k * rows + SUB
            small_ref[at : at + SUB, :] = jnp.zeros((SUB, tile), jnp.float32)
            small_ref[at : at + per_piece, :] = turned[k * per_piece : (k + 1) * per_piece, :]


def pack_body(self_ref, order_ref, inner_ref, slab_ref, send_ref, rows_ref):
    tile = slab_ref.shape[0]
    tiles = order_ref.shape[0]
    place = place_of_tile(order_ref, tiles, self_ref[0])
    row_hot = row_choice(inner_ref[pl.ds(place, 1), :], tile)
    width = slab_ref.shape[1]
    step = min(width, 8 * tile)

    def order_rows(c, _):
        at = pl.ds(pl.multiple_of(c * step, step), step)
        rows_ref[:, at] = split_rows(row_hot, slab_ref[:, at])
        return 0

    lax.fori_loop(0, width // step, order_rows, 0)

    def order_columns(t, _):
        at = pl.ds(pl.multiple_of(order_ref[t] * tile, tile), tile)
        chosen = jnp.broadcast_to(inner_ref[pl.ds(t, 1), :], (SUB, tile))
        for g in range(tile // SUB):
            x = rows_ref[g * SUB : (g + 1) * SUB, at]
            send_ref[t, g * SUB : (g + 1) * SUB, :] = jnp.take_along_axis(x, chosen, axis=1)
        return 0

    lax.fori_loop(0, tiles, order_columns, 0)


def route_body(order_ref, lengths_ref, got_ref, send_ref, first_ref, *, per_piece):
    tiles = order_ref.shape[0]

    def block(e, start):
        for j in range(MOSTT):
            @pl.when(j < lengths_ref[e])
            def _():
                first_ref[start + j] = start
        return start + lengths_ref[e]

    lax.fori_loop(0, lengths_ref.shape[0], block, jnp.int32(0))
    spare = send_ref.shape[1] - MOSTT * SUB

    def fill(d, _):
        if spare:
            send_ref[d, MOSTT * SUB :, :] = jnp.zeros((spare, send_ref.shape[2]), jnp.float32)
        for m in range(MOSTT):
            source = order_ref[jnp.minimum(first_ref[d] + m, tiles - 1)]
            send_ref[d, m * SUB : (m + 1) * SUB, :] = got_ref[source, 0:SUB, :]
            if spare:
                at = MOSTT * SUB + m * per_piece
                send_ref[d, at : at + per_piece, :] = got_ref[source, SUB : SUB + per_piece, :]
        return 0

    lax.fori_loop(0, tiles, fill, 0, unroll=4)


def sweep(s):
    for k in range(SUB):
        inverse = pltpu.reciprocal(s[k][k], approx=False)
        column = [s[max(i, k)][min(i, k)] for i in range(SUB)]
        scaled = [column[i] * inverse for i in range(SUB)]
        for i in range(SUB):
            for j in range(i + 1):
                if i != k and j != k:
                    s[i][j] = s[i][j] - scaled[i] * column[j]
        for i in range(SUB):
            if i != k:
                s[max(i, k)][min(i, k)] = scaled[i]
        s[k][k] = -inverse
    return s


def invert_in_place(m_ref):
    size = m_ref.shape[0]
    lane = lax.broadcasted_iota(jnp.int32, (SUB, size), 1)
    sub = lax.broadcasted_iota(jnp.int32, (SUB, size), 0)

    def panel(p, _):
        row = pl.multiple_of(p * SUB, SUB)
        rows = m_ref[pl.ds(row, SUB), :]
        inside = (lane >= row) & (lane < row + SUB)
        at = [jnp.full((SUB, size), row + j, jnp.int32) for j in range(SUB)]
        columns = [jnp.take_along_axis(rows, at[j], axis=1) for j in range(SUB)]
        s = [
            [jnp.broadcast_to(columns[j][i : i + 1, :], (SUB, size)) for j in range(i + 1)]
            for i in range(SUB)
        ]
        s = sweep(s)
        spread = [
            jnp.where(
                inside,
                jnp.where(lane == row + j, 1.0, 0.0),
                jnp.broadcast_to(rows[j : j + 1, :], (SUB, size)),
            )
            for j in range(SUB)
        ]
        update = []
        for i in range(SUB):
            total = s[i][0] * spread[0]
            for j in range(1, SUB):
                total = total + s[max(i, j)][min(i, j)] * spread[j]
            update.append(total)
        new = -update[0]
        for i in range(1, SUB):
            new = jnp.where(sub == i, -update[i], new)
        for g in range(size // SUB):
            here = m_ref[g * SUB : (g + 1) * SUB, :]
            total = jnp.where(inside, 0.0, here)
            for j in range(SUB):
                total = total + jnp.take_along_axis(here, at[j], axis=1) * update[j]
            m_ref[g * SUB : (g + 1) * SUB, :] = total
        m_ref[pl.ds(row, SUB), :] = new
        return 0

    lax.fori_loop(0, size // SUB, panel, 0)


def block_inverse(f_ref, w01, w02, w12):
    e0, e1, e2 = f_ref[0], f_ref[1], f_ref[2]
    v12 = -dot(w12, e2)
    v11 = e1 - dot_t(v12, w12)
    v02 = -dot(w01, v12) - dot(w02, e2)
    v01 = -dot(w01, v11) - dot_t(w02, v12)
    v00 = e0 - dot_t(v01, w01) - dot_t(v02, w02)
    return (v00, v01, v02), (v01.T, v11, v12), (v02.T, v12.T, e2)


def apply_rows(v_ref, b):
    return dot_t(jnp.concatenate(b, axis=1), v_ref[...])


def pick(position, values):
    chosen = values[0]
    for m in range(1, len(values)):
        chosen = jnp.where(position == m, values[m], chosen)
    return chosen


def factor_body(self_ref, lengths_ref, got_ref, v_ref, b_ref, z_ref, f_ref, o_ref, bs_ref, *, per_piece):
    tile = got_ref.shape[2]
    rhs = b_ref.shape[0]
    pieces = 2 * tile // SUB
    half = tile // 2
    first, length = block_of(lengths_ref, self_ref[0])
    position = self_ref[0] - first
    row = lax.broadcasted_iota(jnp.int32, (tile, tile), 0)
    lane = lax.broadcasted_iota(jnp.int32, (tile, tile), 1)
    for m in range(MOSTT):
        pair_inside = m + 1 < length if m < MOSTT - 1 else m < length
        for k in range(pieces // 2):
            at = slice(k * SUB, (k + 1) * SUB)
            f_ref[m, at, :] = got_ref[k, m * SUB : (m + 1) * SUB, :]
            beside = got_ref[k + pieces // 2, m * SUB : (m + 1) * SUB, :]
            o_ref[m, at, :] = jnp.where(pair_inside, beside, 0.0)
        own = f_ref[m]
        if sides_fit(tile, rhs):
            low = own[half : half + rhs, :]
            high = pltpu.roll(own[half + rhs :, :], half, 1)
            side = jnp.where(lane[:rhs, :] < half, low, high)
            own = jnp.where((row >= half) & (lane < half), own.T, own)
            bs_ref[m] = jnp.where(m < length, side, 0.0)
        else:
            for k in range(pieces):
                start = MOSTT * SUB + m * per_piece
                part = got_ref[k, start : start + per_piece, :]
                bs_ref[m, k * per_piece : (k + 1) * per_piece, :] = jnp.where(m < length, part, 0.0)
        f_ref[m] = jnp.where(m < length, own, jnp.where(row == lane, 1.0, 0.0))
    a01 = o_ref[0]
    a12 = o_ref[1]
    a20 = o_ref[2]
    a10 = a01.T
    invert_in_place(f_ref.at[0])
    w01 = dot(f_ref[0], a01)
    w02 = dot_t(f_ref[0], a20)
    f_ref[1] = f_ref[1] - dot(a10, w01)
    s12 = a12 - dot(a10, w02)
    invert_in_place(f_ref.at[1])
    w12 = dot(f_ref[1], s12)
    f_ref[2] = f_ref[2] - dot(a20, w02) - dot(s12.T, w12)
    invert_in_place(f_ref.at[2])
    rows = block_inverse(f_ref, w01, w02, w12)
    for m in range(MOSTT):
        v_ref[:, m * tile : (m + 1) * tile] = pick(position, [rows[p][m] for p in range(MOSTT)])
    b = [bs_ref[m] for m in range(MOSTT)]
    b_ref[...] = pick(position, b)
    z_ref[...] = apply_rows(v_ref, b)


def arrange_body(order_ref, got_ref, slab_ref, sems):
    tiles = order_ref.shape[0]
    tile = got_ref.shape[1]
    copies = [
        pltpu.make_async_copy(
            got_ref.at[order_ref[t]], slab_ref.at[t * tile : (t + 1) * tile, :], sems.at[t]
        )
        for t in range(tiles)
    ]
    for copy in copies:
        copy.start()
    for copy in copies:
        copy.wait()


def residual_body(self_ref, order_ref, got_ref, b_ref, *rest, flips):
    part_refs, r_ref, x_ref = rest[:-2], rest[-2], rest[-1]
    _, tile = b_ref.shape
    tiles = order_ref.shape[0]
    me = self_ref[0]
    j = 0
    for part_ref in part_refs:
        for i in range(part_ref.shape[0]):
            at = pl.multiple_of(order_ref[me ^ flips[j]] * tile, tile)
            x_ref[:, pl.ds(at, tile)] = part_ref[i]
            j += 1
    group = 8
    total = b_ref[...]
    for c in range(tiles // group):
        x = x_ref[:, c * group * tile : (c + 1) * group * tile]
        g = got_ref[c * group : (c + 1) * group].reshape(group * tile, tile)
        total = total - dot(x, g)
    r_ref[...] = total


def finish_body(self_ref, lengths_ref, v_ref, z_ref, *rest):
    near_refs, out_ref, all_ref = rest[:-2], rest[-2], rest[-1]
    place = self_ref[0]
    first, length = block_of(lengths_ref, place)
    position = place - first
    for i, near_ref in enumerate(near_refs):
        all_ref[i] = near_ref[...]
    b = []
    for m in range(MOSTT):
        r = all_ref[jnp.clip(MOSTT - 1 + m - position, 0, len(near_refs) - 1)]
        b.append(jnp.where(m < length, r, 0.0))
    out_ref[...] = z_ref[...] + apply_rows(v_ref, b)


def shift(value, steps):
    count = lax.axis_size(AXES)
    pairs = [(s, (s + steps) % count) for s in range(count)]
    return lax.ppermute(value, AXES, pairs)


def exchange(value, rows):
    lanes = value.shape[-1]
    moved = lax.all_to_all(value.reshape(-1, lanes), AXES, 0, 0, tiled=True)
    return moved.reshape(-1, rows, lanes)


def small_enough(dims):
    return math.prod(dims) <= 1 << 19


def swap(value, bit):
    count = lax.axis_size(AXES)
    return lax.ppermute(value, AXES, [(s, s ^ bit) for s in range(count)])


def spread(value):
    count_x, count_y = lax.axis_size("gx"), lax.axis_size("gy")
    assert count_x & (count_x - 1) == 0 and count_y & (count_y - 1) == 0
    low = 1 << ((count_y.bit_length() - 1) // 2)
    held, flips = value[None], [0]
    bits = [count_y << i for i in range(1, count_x.bit_length() - 1)]
    bits += [1 << i for i in range(low.bit_length() - 1)]
    for bit in bits:
        held = jnp.concatenate([held, swap(held, bit)], axis=0)
        flips += [f ^ bit for f in flips]
    across = [low * i for i in range(1, count_y // low)]
    parts = [held] + [swap(held, bit) for bit in across]
    held = jnp.concatenate(parts, axis=0)
    flips += [f ^ bit for bit in across for f in flips]
    if count_x > 1:
        parts = [held, swap(held, count_y)]
        flips += [f ^ count_y for f in flips]
    else:
        parts = [held]
    return parts, tuple(flips)


def body(normal_matrix, right_sides, tile_order, inner_order, block_lengths):
    f32 = jnp.float32
    tile = normal_matrix.shape[0]
    rhs = right_sides.shape[1]
    tiles = tile_order.shape[0]
    per_piece = rhs // (2 * tile // SUB)
    fit = sides_fit(tile, rhs)
    me = lax.axis_index(AXES).astype(jnp.int32).reshape(1)
    smem = pl.BlockSpec(memory_space=pltpu.SMEM)
    vmem = pl.BlockSpec(memory_space=pltpu.VMEM)
    hbm = pl.BlockSpec(memory_space=pl.ANY)
    shape = lambda *dims: jax.ShapeDtypeStruct(dims, f32)

    def held(*dims):
        return pltpu.VMEM(dims, f32) if small_enough(dims) else shape(*dims)

    def hold(x):
        return pltpu.with_memory_space_constraint(x, pltpu.VMEM) if small_enough(x.shape) else x


    slab_bytes = 4 * normal_matrix.size
    room = lambda slabs: pltpu.CompilerParams(vmem_limit_bytes=int(slabs * slab_bytes) + (4 << 20))

    small_rows = SUB if fit else 2 * SUB
    small = pl.pallas_call(
        near_body,
        out_shape=held(tiles * small_rows, tile),
        in_specs=[smem, smem, smem, vmem, vmem, hbm],
        out_specs=vmem,
        scratch_shapes=[pltpu.VMEM((2, tile, tile), f32), pltpu.SemaphoreType.DMA((2,))],
        name="near",
    )(me, tile_order, block_lengths, inner_order, right_sides.T, normal_matrix)
    small_got = exchange(small, small_rows)
    tiles_out = pl.pallas_call(
        pack_body,
        out_shape=shape(tiles, tile, tile),
        in_specs=[smem, smem, vmem, vmem],
        out_specs=vmem,
        scratch_shapes=[pltpu.VMEM(normal_matrix.shape, f32)],
        name="pack",
    )(me, tile_order, inner_order, normal_matrix)
    routed_rows = MOSTT * SUB + (0 if fit else -(-MOSTT * per_piece // SUB) * SUB)
    routed = pl.pallas_call(
        lambda *refs: route_body(*refs, per_piece=per_piece),
        out_shape=held(tiles, routed_rows, tile),
        in_specs=[smem, smem, vmem],
        out_specs=vmem,
        scratch_shapes=[pltpu.SMEM((tiles,), jnp.int32)],
        name="route",
    )(tile_order, block_lengths, hold(small_got))
    block_parts = exchange(routed, routed_rows)
    tiles_got = exchange(tiles_out, tile)

    inverse_rows, own_sides, z = pl.pallas_call(
        lambda *refs: factor_body(*refs, per_piece=per_piece),
        out_shape=(held(tile, MOSTT * tile), held(rhs, tile), held(rhs, tile)),
        in_specs=[smem, smem, vmem],
        out_specs=(vmem, vmem, vmem),
        scratch_shapes=[
            pltpu.VMEM((MOSTT, tile, tile), f32),
            pltpu.VMEM((MOSTT, tile, tile), f32),
            pltpu.VMEM((MOSTT, rhs, tile), f32),
        ],
        name="factor",
        compiler_params=room(1),
    )(me, block_lengths, hold(block_parts))

    iterate, flips = spread(z)
    slab = pl.pallas_call(
        arrange_body,
        out_shape=shape(tiles * tile, tile),
        in_specs=[smem, vmem],
        out_specs=hbm,
        scratch_shapes=[pltpu.SemaphoreType.DMA((tiles,))],
        name="arrange",
    compiler_params=room(1),
    )(tile_order, hold(tiles_got))
    residual = pl.pallas_call(
        lambda *refs: residual_body(*refs, flips=flips),
        out_shape=held(rhs, tile),
        in_specs=[smem, smem, vmem, vmem] + [vmem] * len(iterate),
        out_specs=vmem,
        scratch_shapes=[pltpu.VMEM((rhs, tiles * tile), f32)],
        name="residual",
        compiler_params=room(3),
    )(me, tile_order, hold(tiles_got), hold(own_sides), *map(hold, iterate))
    near = [
        residual if o == 0 else shift(residual, -o) for o in range(1 - MOSTT, MOSTT)
    ]
    solved = pl.pallas_call(
        finish_body,
        out_shape=shape(rhs, tile),
        in_specs=[smem, smem, vmem, vmem] + [vmem] * len(near),
        out_specs=vmem,
        scratch_shapes=[pltpu.VMEM((len(near), rhs, tile), f32)],
        name="finish",
        compiler_params=room(0.5),
    )(me, block_lengths, hold(inverse_rows), hold(z), *map(hold, near))
    return slab, solved.T


def solution(mesh):
    placed = (P(AXES, None), P(AXES, None), P(), P(), P())
    return jax.shard_map(
        body,
        mesh=mesh,
        in_specs=placed,
        out_specs=(P(None, AXES), P(AXES, None)),
        check_vma=False,
    )
```

```python
import math

import jax
import jax.numpy as jnp
from jax import lax
from jax.experimental import pallas as pl
from jax.experimental.pallas import tpu as pltpu
from jax.sharding import PartitionSpec as P


MOSTT = 3
AXES = ("gx", "gy")
SUB = 8
HIGHEST = lax.Precision.HIGHEST


def dot(a, b, contract=((1,), (0,))):
    return lax.dot_general(
        a, b, (contract, ((), ())), precision=HIGHEST, preferred_element_type=jnp.float32
    )


def dot_t(a, b):
    return dot(a, b, ((1,), (1,)))


def one_pass(a, b):
    return lax.dot_general(a, b, (((1,), (0,)), ((), ())), preferred_element_type=jnp.float32)


def place_of_tile(order_ref, tiles, old_tile):
    def step(t, found):
        return jnp.where(order_ref[t] == old_tile, t, found)

    return lax.fori_loop(0, tiles, step, jnp.int32(0), unroll=8)


def block_of(lengths_ref, place):
    def step(e, carry):
        start, first, length = carry
        here = (start <= place) & (place < start + lengths_ref[e])
        first = jnp.where(here, start, first)
        length = jnp.where(here, lengths_ref[e], length)
        return start + lengths_ref[e], first, length

    zero = jnp.int32(0)
    _, first, length = lax.fori_loop(
        0, lengths_ref.shape[0], step, (zero, zero, zero + 1), unroll=8
    )
    return first, length


def split_rows(hot, x):
    high = x.astype(jnp.bfloat16)
    rest = x - high.astype(jnp.float32)
    middle = rest.astype(jnp.bfloat16)
    low = (rest - middle.astype(jnp.float32)).astype(jnp.bfloat16)
    return (one_pass(hot, low) + one_pass(hot, middle)) + one_pass(hot, high)


def row_choice(inner_row, tile):
    hot = jnp.where(lax.broadcasted_iota(jnp.int32, (tile, tile), 0) == inner_row, 1.0, 0.0)
    return hot.T.astype(jnp.bfloat16)


def sides_fit(tile, rhs):
    return 4 * rhs == tile


def near_body(self_ref, order_ref, lengths_ref, sides_ref, slab_ref, small_ref, near_ref, sems):
    tile = slab_ref.shape[0]
    tiles = order_ref.shape[0]
    rhs = sides_ref.shape[0]
    me = self_ref[0]
    pieces = 2 * tile // SUB
    rows = small_ref.shape[0] // tiles
    half = tile // 2
    fit = sides_fit(tile, rhs)

    def fetch(i, old_tile):
        at = pl.ds(pl.multiple_of(old_tile * tile, tile), tile)
        target = small_ref.at[i * tile : (i + 1) * tile, :] if fit else near_ref.at[i]
        copy = pltpu.make_async_copy(slab_ref.at[:, at], target, sems.at[i])
        copy.start()
        return copy

    own = fetch(0, me)
    place = place_of_tile(order_ref, tiles, me)
    first, _ = block_of(lengths_ref, place)
    position = place - first
    after = jnp.where(position == MOSTT - 1, 0, position + 1)
    beside = fetch(1, order_ref[jnp.minimum(first + after, tiles - 1)])
    if small_ref.shape[0] > pieces * rows:
        small_ref[pieces * rows :, :] = jnp.zeros((small_ref.shape[0] - pieces * rows, tile), jnp.float32)
    own.wait()
    if fit:
        sides = sides_ref[...]
        lane = lax.broadcasted_iota(jnp.int32, (tile - half, tile), 1)
        extra = jnp.concatenate([sides, pltpu.roll(sides, half, 1)], axis=0)
        small_ref[half:tile, :] = jnp.where(lane < half, extra, small_ref[half:tile, :])
        beside.wait()
    else:
        beside.wait()
        per_piece = rhs // pieces
        for k in range(pieces):
            at = k * rows
            start = k * SUB % tile
            small_ref[at : at + SUB, :] = near_ref[k * SUB // tile, start : start + SUB, :]
            small_ref[at + SUB : at + 2 * SUB, :] = jnp.zeros((SUB, tile), jnp.float32)
            small_ref[at + SUB : at + SUB + per_piece, :] = sides_ref[k * per_piece : (k + 1) * per_piece, :]


def pack_body(self_ref, order_ref, inner_ref, slab_ref, send_ref, rows_ref):
    tile = slab_ref.shape[0]
    tiles = order_ref.shape[0]
    place = place_of_tile(order_ref, tiles, self_ref[0])
    row_hot = row_choice(inner_ref[pl.ds(place, 1), :], tile)
    width = slab_ref.shape[1]
    step = min(width, 8 * tile)

    def order_rows(c, _):
        at = pl.ds(pl.multiple_of(c * step, step), step)
        rows_ref[:, at] = split_rows(row_hot, slab_ref[:, at])
        return 0

    lax.fori_loop(0, width // step, order_rows, 0)

    def order_columns(t, _):
        at = pl.ds(pl.multiple_of(order_ref[t] * tile, tile), tile)
        chosen = jnp.broadcast_to(inner_ref[pl.ds(t, 1), :], (SUB, tile))
        for g in range(tile // SUB):
            x = rows_ref[g * SUB : (g + 1) * SUB, at]
            send_ref[t, g * SUB : (g + 1) * SUB, :] = jnp.take_along_axis(x, chosen, axis=1)
        return 0

    lax.fori_loop(0, tiles, order_columns, 0)


def route_body(order_ref, lengths_ref, got_ref, send_ref, first_ref, *, per_piece):
    tiles = order_ref.shape[0]

    def block(e, start):
        for j in range(MOSTT):
            first_ref[start + j] = start
        return start + lengths_ref[e]

    lax.fori_loop(0, lengths_ref.shape[0], block, jnp.int32(0), unroll=8)
    spare = send_ref.shape[1] - MOSTT * SUB

    def fill(d, _):
        if spare:
            send_ref[d, MOSTT * SUB :, :] = jnp.zeros((spare, send_ref.shape[2]), jnp.float32)
        for m in range(MOSTT):
            source = order_ref[jnp.minimum(first_ref[d] + m, tiles - 1)]
            send_ref[d, m * SUB : (m + 1) * SUB, :] = got_ref[source, 0:SUB, :]
            if spare:
                at = MOSTT * SUB + m * per_piece
                send_ref[d, at : at + per_piece, :] = got_ref[source, SUB : SUB + per_piece, :]
        return 0

    lax.fori_loop(0, tiles, fill, 0, unroll=4)


def sweep(s):
    for k in range(SUB):
        inverse = pltpu.reciprocal(s[k][k], approx=False)
        column = [s[max(i, k)][min(i, k)] for i in range(SUB)]
        scaled = [column[i] * inverse for i in range(SUB)]
        for i in range(SUB):
            for j in range(i + 1):
                if i != k and j != k:
                    s[i][j] = s[i][j] - scaled[i] * column[j]
        for i in range(SUB):
            if i != k:
                s[max(i, k)][min(i, k)] = scaled[i]
        s[k][k] = -inverse
    return s


def invert_in_place(m_ref):
    size = m_ref.shape[0]
    lane = lax.broadcasted_iota(jnp.int32, (SUB, size), 1)
    sub = lax.broadcasted_iota(jnp.int32, (SUB, size), 0)

    def panel(p, _):
        row = pl.multiple_of(p * SUB, SUB)
        rows = m_ref[pl.ds(row, SUB), :]
        inside = (lane >= row) & (lane < row + SUB)
        at = [jnp.full((SUB, size), row + j, jnp.int32) for j in range(SUB)]
        columns = [jnp.take_along_axis(rows, at[j], axis=1) for j in range(SUB)]
        s = [
            [jnp.broadcast_to(columns[j][i : i + 1, :], (SUB, size)) for j in range(i + 1)]
            for i in range(SUB)
        ]
        s = sweep(s)
        spread = [
            jnp.where(
                inside,
                jnp.where(lane == row + j, 1.0, 0.0),
                jnp.broadcast_to(rows[j : j + 1, :], (SUB, size)),
            )
            for j in range(SUB)
        ]
        update = []
        for i in range(SUB):
            total = s[i][0] * spread[0]
            for j in range(1, SUB):
                total = total + s[max(i, j)][min(i, j)] * spread[j]
            update.append(total)
        new = -update[0]
        for i in range(1, SUB):
            new = jnp.where(sub == i, -update[i], new)
        for g in range(size // SUB):
            here = m_ref[g * SUB : (g + 1) * SUB, :]
            total = jnp.where(inside, 0.0, here)
            for j in range(SUB):
                total = total + jnp.take_along_axis(here, at[j], axis=1) * update[j]
            m_ref[g * SUB : (g + 1) * SUB, :] = total
        m_ref[pl.ds(row, SUB), :] = new
        return 0

    lax.fori_loop(0, size // SUB, panel, 0)


def block_inverse(f_ref, w01, w02, w12):
    e0, e1, e2 = f_ref[0], f_ref[1], f_ref[2]
    v12 = -dot(w12, e2)
    v11 = e1 - dot_t(v12, w12)
    v02 = -dot(w01, v12) - dot(w02, e2)
    v01 = -dot(w01, v11) - dot_t(w02, v12)
    v00 = e0 - dot_t(v01, w01) - dot_t(v02, w02)
    return (v00, v01, v02), (v01.T, v11, v12), (v02.T, v12.T, e2)


def apply_rows(v_ref, b):
    return dot_t(jnp.concatenate(b, axis=1), v_ref[...])


def pick(position, values):
    chosen = values[0]
    for m in range(1, len(values)):
        chosen = jnp.where(position == m, values[m], chosen)
    return chosen


def factor_body(self_ref, lengths_ref, inner_ref, got_ref, v_ref, b_ref, z_ref, f_ref, o_ref, bs_ref, *, per_piece):
    tile = got_ref.shape[2]
    rhs = b_ref.shape[0]
    pieces = 2 * tile // SUB
    half = tile // 2
    first, length = block_of(lengths_ref, self_ref[0])
    position = self_ref[0] - first
    row = lax.broadcasted_iota(jnp.int32, (tile, tile), 0)
    lane = lax.broadcasted_iota(jnp.int32, (tile, tile), 1)
    inner = [inner_ref[pl.ds(jnp.minimum(first + m, inner_ref.shape[0] - 1), 1), :] for m in range(MOSTT)]
    hot = [row_choice(order, tile) for order in inner]

    def ordered(x, m, n):
        moved = split_rows(hot[m], x)
        return jnp.take_along_axis(moved, jnp.broadcast_to(inner[n], (tile, tile)), axis=1)

    for m in range(MOSTT):
        pair_inside = m + 1 < length if m < MOSTT - 1 else m < length
        for k in range(pieces // 2):
            at = slice(k * SUB, (k + 1) * SUB)
            f_ref[m, at, :] = got_ref[k, m * SUB : (m + 1) * SUB, :]
            o_ref[m, at, :] = got_ref[k + pieces // 2, m * SUB : (m + 1) * SUB, :]
        o_ref[m] = jnp.where(pair_inside, ordered(o_ref[m], m, (m + 1) % MOSTT), 0.0)
        own = f_ref[m]
        if sides_fit(tile, rhs):
            low = own[half : half + rhs, :]
            high = pltpu.roll(own[half + rhs :, :], half, 1)
            side = jnp.where(lane[:rhs, :] < half, low, high)
            own = jnp.where((row >= half) & (lane < half), own.T, own)
            bs_ref[m] = side
        else:
            for k in range(pieces):
                start = MOSTT * SUB + m * per_piece
                part = got_ref[k, start : start + per_piece, :]
                bs_ref[m, k * per_piece : (k + 1) * per_piece, :] = part
        side = jnp.take_along_axis(bs_ref[m], jnp.broadcast_to(inner[m], (rhs, tile)), axis=1)
        bs_ref[m] = jnp.where(m < length, side, 0.0)
        f_ref[m] = jnp.where(m < length, ordered(own, m, m), jnp.where(row == lane, 1.0, 0.0))
    a01 = o_ref[0]
    a12 = o_ref[1]
    a20 = o_ref[2]
    a10 = a01.T
    invert_in_place(f_ref.at[0])
    w01 = dot(f_ref[0], a01)
    w02 = dot_t(f_ref[0], a20)
    f_ref[1] = f_ref[1] - dot(a10, w01)
    s12 = a12 - dot(a10, w02)
    invert_in_place(f_ref.at[1])
    w12 = dot(f_ref[1], s12)
    f_ref[2] = f_ref[2] - dot(a20, w02) - dot(s12.T, w12)
    invert_in_place(f_ref.at[2])
    rows = block_inverse(f_ref, w01, w02, w12)
    for m in range(MOSTT):
        v_ref[:, m * tile : (m + 1) * tile] = pick(position, [rows[p][m] for p in range(MOSTT)])
    b = [bs_ref[m] for m in range(MOSTT)]
    b_ref[...] = pick(position, b)
    z_ref[...] = apply_rows(v_ref, b)


def arrange_body(order_ref, got_ref, slab_ref, sems):
    tiles = order_ref.shape[0]
    tile = got_ref.shape[1]
    copies = [
        pltpu.make_async_copy(
            got_ref.at[order_ref[t]], slab_ref.at[t * tile : (t + 1) * tile, :], sems.at[t]
        )
        for t in range(tiles)
    ]
    for copy in copies:
        copy.start()
    for copy in copies:
        copy.wait()


def residual_body(self_ref, order_ref, got_ref, b_ref, part_ref, r_ref, x_ref, tiles_ref, *, flips):
    tile = b_ref.shape[1]
    me = self_ref[0]
    for i, flip in enumerate(flips):
        x_ref[:, i * tile : (i + 1) * tile] = part_ref[i]
        tiles_ref[i * tile : (i + 1) * tile, :] = got_ref[order_ref[me ^ flip]]
    width = x_ref.shape[1]
    group = min(width, 8 * tile)
    total = b_ref[...]
    for c in range(0, width, group):
        total = total - dot(x_ref[:, c : c + group], tiles_ref[c : c + group, :])
    r_ref[...] = total


def finish_body(self_ref, lengths_ref, v_ref, z_ref, *rest):
    near_refs, out_ref, all_ref = rest[:-2], rest[-2], rest[-1]
    place = self_ref[0]
    first, length = block_of(lengths_ref, place)
    position = place - first
    for i, near_ref in enumerate(near_refs):
        all_ref[i] = near_ref[...]
    b = []
    for m in range(MOSTT):
        r = all_ref[jnp.clip(MOSTT - 1 + m - position, 0, len(near_refs) - 1)]
        b.append(jnp.where(m < length, r, 0.0))
    out_ref[...] = z_ref[...] + apply_rows(v_ref, b)


def shift(value, steps):
    count = lax.axis_size(AXES)
    pairs = [(s, (s + steps) % count) for s in range(count)]
    return lax.ppermute(value, AXES, pairs)


def exchange(value, rows):
    lanes = value.shape[-1]
    moved = lax.all_to_all(value.reshape(-1, lanes), AXES, 0, 0, tiled=True)
    return moved.reshape(-1, rows, lanes)


def small_enough(dims):
    return math.prod(dims) <= 1 << 19


def swap(value, bit):
    count = lax.axis_size(AXES)
    return lax.ppermute(value, AXES, [(s, s ^ bit) for s in range(count)])


def spread(value):
    count_x, count_y = lax.axis_size("gx"), lax.axis_size("gy")
    assert count_x & (count_x - 1) == 0 and count_y & (count_y - 1) == 0
    low = 1 << ((count_y.bit_length() - 1) // 2)
    held, flips = value[None], [0]
    bits = [count_y << i for i in range(1, count_x.bit_length() - 1)]
    bits += [1 << i for i in range(low.bit_length() - 1)]
    for bit in bits:
        held = jnp.concatenate([held, swap(held, bit)], axis=0)
        flips += [f ^ bit for f in flips]
    across = [low * i for i in range(1, count_y // low)]
    parts = [held] + [swap(held, bit) for bit in across]
    held = jnp.concatenate(parts, axis=0)
    flips += [f ^ bit for bit in across for f in flips]
    if count_x > 1:
        parts = [held, swap(held, count_y)]
        flips += [f ^ count_y for f in flips]
    else:
        parts = [held]
    return parts, tuple(flips)


def body(normal_matrix, right_sides, tile_order, inner_order, block_lengths):
    f32 = jnp.float32
    tile = normal_matrix.shape[0]
    rhs = right_sides.shape[1]
    tiles = tile_order.shape[0]
    per_piece = rhs // (2 * tile // SUB)
    fit = sides_fit(tile, rhs)
    me = lax.axis_index(AXES).astype(jnp.int32).reshape(1)
    smem = pl.BlockSpec(memory_space=pltpu.SMEM)
    vmem = pl.BlockSpec(memory_space=pltpu.VMEM)
    hbm = pl.BlockSpec(memory_space=pl.ANY)
    shape = lambda *dims: jax.ShapeDtypeStruct(dims, f32)

    def held(*dims):
        return pltpu.VMEM(dims, f32) if small_enough(dims) else shape(*dims)

    def hold(x):
        return pltpu.with_memory_space_constraint(x, pltpu.VMEM) if small_enough(x.shape) else x


    slab_bytes = 4 * normal_matrix.size
    room = lambda slabs: pltpu.CompilerParams(vmem_limit_bytes=int(slabs * slab_bytes) + (4 << 20))

    small_rows = SUB if fit else 2 * SUB
    small = pl.pallas_call(
        near_body,
        out_shape=held(tiles * small_rows, tile),
        in_specs=[smem, smem, smem, vmem, hbm],
        out_specs=vmem,
        scratch_shapes=[pltpu.VMEM((2, tile, tile), f32), pltpu.SemaphoreType.DMA((2,))],
        name="near",
    )(me, tile_order, block_lengths, right_sides.T, normal_matrix)
    small_got = exchange(small, small_rows)
    tiles_out = pl.pallas_call(
        pack_body,
        out_shape=shape(tiles, tile, tile),
        in_specs=[smem, smem, vmem, vmem],
        out_specs=vmem,
        scratch_shapes=[pltpu.VMEM(normal_matrix.shape, f32)],
        name="pack",
    )(me, tile_order, inner_order, normal_matrix)
    routed_rows = MOSTT * SUB + (0 if fit else -(-MOSTT * per_piece // SUB) * SUB)
    routed = pl.pallas_call(
        lambda *refs: route_body(*refs, per_piece=per_piece),
        out_shape=held(tiles, routed_rows, tile),
        in_specs=[smem, smem, vmem],
        out_specs=vmem,
        scratch_shapes=[pltpu.SMEM((tiles + MOSTT,), jnp.int32)],
        name="route",
    )(tile_order, block_lengths, hold(small_got))
    block_parts = exchange(routed, routed_rows)
    tiles_got = exchange(tiles_out, tile)

    inverse_rows, own_sides, z = pl.pallas_call(
        lambda *refs: factor_body(*refs, per_piece=per_piece),
        out_shape=(held(tile, MOSTT * tile), held(rhs, tile), held(rhs, tile)),
        in_specs=[smem, smem, vmem, vmem],
        out_specs=(vmem, vmem, vmem),
        scratch_shapes=[
            pltpu.VMEM((MOSTT, tile, tile), f32),
            pltpu.VMEM((MOSTT, tile, tile), f32),
            pltpu.VMEM((MOSTT, rhs, tile), f32),
        ],
        name="factor",
        compiler_params=room(1),
    )(me, block_lengths, inner_order, hold(block_parts))

    iterate, flips = spread(z)
    slab = pl.pallas_call(
        arrange_body,
        out_shape=shape(tiles * tile, tile),
        in_specs=[smem, vmem],
        out_specs=hbm,
        scratch_shapes=[pltpu.SemaphoreType.DMA((tiles,))],
        name="arrange",
    compiler_params=room(1),
    )(tile_order, hold(tiles_got))

    def subtract(left, part, chosen):
        return pl.pallas_call(
            lambda *refs: residual_body(*refs, flips=chosen),
            out_shape=held(rhs, tile),
            in_specs=[smem, smem, vmem, vmem, vmem],
            out_specs=vmem,
            scratch_shapes=[
                pltpu.VMEM((rhs, len(chosen) * tile), f32),
                pltpu.VMEM((len(chosen) * tile, tile), f32),
            ],
            name="residual",
            compiler_params=room(3),
        )(me, tile_order, hold(tiles_got), hold(left), hold(part))

    residual = own_sides
    for part in iterate[:-1]:
        residual = subtract(residual, part, flips[: part.shape[0]])
        flips = flips[part.shape[0] :]
    residual = subtract(residual, iterate[-1], flips)
    near = [
        residual if o == 0 else shift(residual, -o) for o in range(1 - MOSTT, MOSTT)
    ]
    solved = pl.pallas_call(
        finish_body,
        out_shape=shape(rhs, tile),
        in_specs=[smem, smem, vmem, vmem] + [vmem] * len(near),
        out_specs=vmem,
        scratch_shapes=[pltpu.VMEM((len(near), rhs, tile), f32)],
        name="finish",
        compiler_params=room(0.5),
    )(me, block_lengths, hold(inverse_rows), hold(z), *map(hold, near))
    return slab, solved.T


def solution(mesh):
    placed = (P(AXES, None), P(AXES, None), P(), P(), P())
    return jax.shard_map(
        body,
        mesh=mesh,
        in_specs=placed,
        out_specs=(P(None, AXES), P(AXES, None)),
        check_vma=False,
    )
```

```python
import math

import jax
import jax.numpy as jnp
from jax import lax
from jax.experimental import pallas as pl
from jax.experimental.pallas import tpu as pltpu
from jax.sharding import PartitionSpec as P


MOSTT = 3
AXES = ("gx", "gy")
SUB = 8
HIGHEST = lax.Precision.HIGHEST


def dot(a, b, contract=((1,), (0,))):
    return lax.dot_general(
        a, b, (contract, ((), ())), precision=HIGHEST, preferred_element_type=jnp.float32
    )


def dot_t(a, b):
    return dot(a, b, ((1,), (1,)))


def one_pass(a, b):
    return lax.dot_general(a, b, (((1,), (0,)), ((), ())), preferred_element_type=jnp.float32)


def place_of_tile(order_ref, tiles, old_tile):
    def step(t, found):
        return jnp.where(order_ref[t] == old_tile, t, found)

    return lax.fori_loop(0, tiles, step, jnp.int32(0), unroll=8)


def block_of(lengths_ref, place):
    def step(e, carry):
        start, first, length = carry
        here = (start <= place) & (place < start + lengths_ref[e])
        first = jnp.where(here, start, first)
        length = jnp.where(here, lengths_ref[e], length)
        return start + lengths_ref[e], first, length

    zero = jnp.int32(0)
    _, first, length = lax.fori_loop(
        0, lengths_ref.shape[0], step, (zero, zero, zero + 1), unroll=8
    )
    return first, length


def split_rows(hot, x):
    high = x.astype(jnp.bfloat16)
    rest = x - high.astype(jnp.float32)
    middle = rest.astype(jnp.bfloat16)
    low = (rest - middle.astype(jnp.float32)).astype(jnp.bfloat16)
    return (one_pass(hot, low) + one_pass(hot, middle)) + one_pass(hot, high)


def row_choice(inner_row, tile):
    hot = jnp.where(lax.broadcasted_iota(jnp.int32, (tile, tile), 0) == inner_row, 1.0, 0.0)
    return hot.T.astype(jnp.bfloat16)


def sides_fit(tile, rhs):
    return 4 * rhs == tile


def near_body(self_ref, order_ref, lengths_ref, sides_ref, slab_ref, small_ref, near_ref, sems):
    tile = slab_ref.shape[0]
    tiles = order_ref.shape[0]
    rhs = sides_ref.shape[0]
    me = self_ref[0]
    pieces = 2 * tile // SUB
    rows = small_ref.shape[0] // tiles
    half = tile // 2
    fit = sides_fit(tile, rhs)

    def fetch(i, old_tile):
        at = pl.ds(pl.multiple_of(old_tile * tile, tile), tile)
        target = small_ref.at[i * tile : (i + 1) * tile, :] if fit else near_ref.at[i]
        copy = pltpu.make_async_copy(slab_ref.at[:, at], target, sems.at[i])
        copy.start()
        return copy

    own = fetch(0, me)
    place = place_of_tile(order_ref, tiles, me)
    first, _ = block_of(lengths_ref, place)
    position = place - first
    after = jnp.where(position == MOSTT - 1, 0, position + 1)
    beside = fetch(1, order_ref[jnp.minimum(first + after, tiles - 1)])
    if small_ref.shape[0] > pieces * rows:
        small_ref[pieces * rows :, :] = jnp.zeros((small_ref.shape[0] - pieces * rows, tile), jnp.float32)
    own.wait()
    if fit:
        sides = sides_ref[...]
        lane = lax.broadcasted_iota(jnp.int32, (tile - half, tile), 1)
        extra = jnp.concatenate([sides, pltpu.roll(sides, half, 1)], axis=0)
        small_ref[half:tile, :] = jnp.where(lane < half, extra, small_ref[half:tile, :])
        beside.wait()
    else:
        beside.wait()
        per_piece = rhs // pieces
        for k in range(pieces):
            at = k * rows
            start = k * SUB % tile
            small_ref[at : at + SUB, :] = near_ref[k * SUB // tile, start : start + SUB, :]
            small_ref[at + SUB : at + 2 * SUB, :] = jnp.zeros((SUB, tile), jnp.float32)
            small_ref[at + SUB : at + SUB + per_piece, :] = sides_ref[k * per_piece : (k + 1) * per_piece, :]


def pack_body(self_ref, order_ref, inner_ref, slab_ref, send_ref, rows_ref):
    tile = slab_ref.shape[0]
    tiles = order_ref.shape[0]
    place = place_of_tile(order_ref, tiles, self_ref[0])
    row_hot = row_choice(inner_ref[pl.ds(place, 1), :], tile)
    width = slab_ref.shape[1]
    step = min(width, 8 * tile)

    def order_rows(c, _):
        at = pl.ds(pl.multiple_of(c * step, step), step)
        rows_ref[:, at] = split_rows(row_hot, slab_ref[:, at])
        return 0

    lax.fori_loop(0, width // step, order_rows, 0)

    def order_columns(t, _):
        at = pl.ds(pl.multiple_of(order_ref[t] * tile, tile), tile)
        chosen = jnp.broadcast_to(inner_ref[pl.ds(t, 1), :], (SUB, tile))
        for g in range(tile // SUB):
            x = rows_ref[g * SUB : (g + 1) * SUB, at]
            send_ref[t, g * SUB : (g + 1) * SUB, :] = jnp.take_along_axis(x, chosen, axis=1)
        return 0

    lax.fori_loop(0, tiles, order_columns, 0)


def route_body(order_ref, lengths_ref, got_ref, send_ref, first_ref, *, per_piece):
    tiles = order_ref.shape[0]

    def block(e, start):
        for j in range(MOSTT):
            first_ref[start + j] = start
        return start + lengths_ref[e]

    lax.fori_loop(0, lengths_ref.shape[0], block, jnp.int32(0), unroll=8)
    spare = send_ref.shape[1] - MOSTT * SUB

    def fill(d, _):
        if spare:
            send_ref[d, MOSTT * SUB :, :] = jnp.zeros((spare, send_ref.shape[2]), jnp.float32)
        for m in range(MOSTT):
            source = order_ref[jnp.minimum(first_ref[d] + m, tiles - 1)]
            send_ref[d, m * SUB : (m + 1) * SUB, :] = got_ref[source, 0:SUB, :]
            if spare:
                at = MOSTT * SUB + m * per_piece
                send_ref[d, at : at + per_piece, :] = got_ref[source, SUB : SUB + per_piece, :]
        return 0

    lax.fori_loop(0, tiles, fill, 0, unroll=4)


def sweep(s):
    for k in range(SUB):
        inverse = pltpu.reciprocal(s[k][k], approx=False)
        column = [s[max(i, k)][min(i, k)] for i in range(SUB)]
        scaled = [column[i] * inverse for i in range(SUB)]
        for i in range(SUB):
            for j in range(i + 1):
                if i != k and j != k:
                    s[i][j] = s[i][j] - scaled[i] * column[j]
        for i in range(SUB):
            if i != k:
                s[max(i, k)][min(i, k)] = scaled[i]
        s[k][k] = -inverse
    return s


def invert_in_place(m_ref):
    size = m_ref.shape[0]
    lane = lax.broadcasted_iota(jnp.int32, (SUB, size), 1)
    sub = lax.broadcasted_iota(jnp.int32, (SUB, size), 0)

    def panel(p, _):
        row = pl.multiple_of(p * SUB, SUB)
        rows = m_ref[pl.ds(row, SUB), :]
        inside = (lane >= row) & (lane < row + SUB)
        at = [jnp.full((SUB, size), row + j, jnp.int32) for j in range(SUB)]
        columns = [jnp.take_along_axis(rows, at[j], axis=1) for j in range(SUB)]
        s = [
            [jnp.broadcast_to(columns[j][i : i + 1, :], (SUB, size)) for j in range(i + 1)]
            for i in range(SUB)
        ]
        s = sweep(s)
        spread = [
            jnp.where(
                inside,
                jnp.where(lane == row + j, 1.0, 0.0),
                jnp.broadcast_to(rows[j : j + 1, :], (SUB, size)),
            )
            for j in range(SUB)
        ]
        update = []
        for i in range(SUB):
            total = s[i][0] * spread[0]
            for j in range(1, SUB):
                total = total + s[max(i, j)][min(i, j)] * spread[j]
            update.append(total)
        new = -update[0]
        for i in range(1, SUB):
            new = jnp.where(sub == i, -update[i], new)
        for g in range(size // SUB):
            here = m_ref[g * SUB : (g + 1) * SUB, :]
            total = jnp.where(inside, 0.0, here)
            for j in range(SUB):
                total = total + jnp.take_along_axis(here, at[j], axis=1) * update[j]
            m_ref[g * SUB : (g + 1) * SUB, :] = total
        m_ref[pl.ds(row, SUB), :] = new
        return 0

    lax.fori_loop(0, size // SUB, panel, 0)


def block_inverse(f_ref, w01, w02, w12):
    e0, e1, e2 = f_ref[0], f_ref[1], f_ref[2]
    v12 = -dot(w12, e2)
    v11 = e1 - dot_t(v12, w12)
    v02 = -dot(w01, v12) - dot(w02, e2)
    v01 = -dot(w01, v11) - dot_t(w02, v12)
    v00 = e0 - dot_t(v01, w01) - dot_t(v02, w02)
    return (v00, v01, v02), (v01.T, v11, v12), (v02.T, v12.T, e2)


def apply_rows(v_ref, b):
    return dot(jnp.concatenate(b, axis=1), v_ref[...])


def pick(position, values):
    chosen = values[0]
    for m in range(1, len(values)):
        chosen = jnp.where(position == m, values[m], chosen)
    return chosen


def factor_body(self_ref, lengths_ref, inner_ref, got_ref, v_ref, b_ref, z_ref, f_ref, o_ref, bs_ref, *, per_piece):
    tile = got_ref.shape[2]
    rhs = b_ref.shape[0]
    pieces = 2 * tile // SUB
    half = tile // 2
    first, length = block_of(lengths_ref, self_ref[0])
    position = self_ref[0] - first
    row = lax.broadcasted_iota(jnp.int32, (tile, tile), 0)
    lane = lax.broadcasted_iota(jnp.int32, (tile, tile), 1)
    inner = [inner_ref[pl.ds(jnp.minimum(first + m, inner_ref.shape[0] - 1), 1), :] for m in range(MOSTT)]
    hot = [row_choice(order, tile) for order in inner]

    def ordered(x, m, n):
        moved = split_rows(hot[m], x)
        return jnp.take_along_axis(moved, jnp.broadcast_to(inner[n], (tile, tile)), axis=1)

    for m in range(MOSTT):
        pair_inside = m + 1 < length if m < MOSTT - 1 else m < length
        for k in range(pieces // 2):
            at = slice(k * SUB, (k + 1) * SUB)
            f_ref[m, at, :] = got_ref[k, m * SUB : (m + 1) * SUB, :]
            o_ref[m, at, :] = got_ref[k + pieces // 2, m * SUB : (m + 1) * SUB, :]
        o_ref[m] = jnp.where(pair_inside, ordered(o_ref[m], m, (m + 1) % MOSTT), 0.0)
        own = f_ref[m]
        if sides_fit(tile, rhs):
            low = own[half : half + rhs, :]
            high = pltpu.roll(own[half + rhs :, :], half, 1)
            side = jnp.where(lane[:rhs, :] < half, low, high)
            own = jnp.where((row >= half) & (lane < half), own.T, own)
            bs_ref[m] = side
        else:
            for k in range(pieces):
                start = MOSTT * SUB + m * per_piece
                part = got_ref[k, start : start + per_piece, :]
                bs_ref[m, k * per_piece : (k + 1) * per_piece, :] = part
        side = jnp.take_along_axis(bs_ref[m], jnp.broadcast_to(inner[m], (rhs, tile)), axis=1)
        bs_ref[m] = jnp.where(m < length, side, 0.0)
        f_ref[m] = jnp.where(m < length, ordered(own, m, m), jnp.where(row == lane, 1.0, 0.0))
    a01 = o_ref[0]
    a12 = o_ref[1]
    a20 = o_ref[2]
    a10 = a01.T
    invert_in_place(f_ref.at[0])
    w01 = dot(f_ref[0], a01)
    w02 = dot_t(f_ref[0], a20)
    f_ref[1] = f_ref[1] - dot(a10, w01)
    s12 = a12 - dot(a10, w02)
    invert_in_place(f_ref.at[1])
    w12 = dot(f_ref[1], s12)
    f_ref[2] = f_ref[2] - dot(a20, w02) - dot(s12.T, w12)
    invert_in_place(f_ref.at[2])
    rows = block_inverse(f_ref, w01, w02, w12)
    for m in range(MOSTT):
        v_ref[m * tile : (m + 1) * tile, :] = pick(position, [rows[m][p] for p in range(MOSTT)])
    b = [bs_ref[m] for m in range(MOSTT)]
    b_ref[...] = pick(position, b)
    z_ref[...] = apply_rows(v_ref, b)


def arrange_body(order_ref, got_ref, slab_ref, sems):
    tiles = order_ref.shape[0]
    tile = got_ref.shape[1]
    copies = [
        pltpu.make_async_copy(
            got_ref.at[order_ref[t]], slab_ref.at[t * tile : (t + 1) * tile, :], sems.at[t]
        )
        for t in range(tiles)
    ]
    for copy in copies:
        copy.start()
    for copy in copies:
        copy.wait()


def residual_body(self_ref, order_ref, got_ref, b_ref, part_ref, r_ref, x_ref, tiles_ref, *, flips):
    tile = b_ref.shape[1]
    me = self_ref[0]
    for i, flip in enumerate(flips):
        x_ref[:, i * tile : (i + 1) * tile] = part_ref[i]
        tiles_ref[i * tile : (i + 1) * tile, :] = got_ref[order_ref[me ^ flip]]
    width = x_ref.shape[1]
    group = min(width, 8 * tile)
    total = b_ref[...]
    for c in range(0, width, group):
        total = total - dot(x_ref[:, c : c + group], tiles_ref[c : c + group, :])
    r_ref[...] = total


def finish_body(self_ref, lengths_ref, v_ref, z_ref, *rest):
    near_refs, out_ref = rest[:-1], rest[-1]
    place = self_ref[0]
    first, length = block_of(lengths_ref, place)
    position = place - first
    around = [near_ref[...] for near_ref in near_refs]
    b = []
    for m in range(MOSTT):
        r = pick(position, [around[MOSTT - 1 + m - p] for p in range(MOSTT)])
        b.append(jnp.where(m < length, r, 0.0))
    out_ref[...] = z_ref[...] + apply_rows(v_ref, b)


def shift(value, steps):
    count = lax.axis_size(AXES)
    pairs = [(s, (s + steps) % count) for s in range(count)]
    return lax.ppermute(value, AXES, pairs)


def exchange(value, rows):
    lanes = value.shape[-1]
    moved = lax.all_to_all(value.reshape(-1, lanes), AXES, 0, 0, tiled=True)
    return moved.reshape(-1, rows, lanes)


def small_enough(dims):
    return math.prod(dims) <= 1 << 19


def swap(value, bit):
    count = lax.axis_size(AXES)
    return lax.ppermute(value, AXES, [(s, s ^ bit) for s in range(count)])


def spread(value):
    count_x, count_y = lax.axis_size("gx"), lax.axis_size("gy")
    assert count_x & (count_x - 1) == 0 and count_y & (count_y - 1) == 0
    low = 1 << ((count_y.bit_length() - 1) // 2)
    held, flips = value[None], [0]
    bits = [count_y << i for i in range(1, count_x.bit_length() - 1)]
    bits += [1 << i for i in range(low.bit_length() - 1)]
    for bit in bits:
        held = jnp.concatenate([held, swap(held, bit)], axis=0)
        flips += [f ^ bit for f in flips]
    across = [low * i for i in range(1, count_y // low)]
    parts = [held] + [swap(held, bit) for bit in across]
    held = jnp.concatenate(parts, axis=0)
    flips += [f ^ bit for bit in across for f in flips]
    if count_x > 1:
        parts = [held, swap(held, count_y)]
        flips += [f ^ count_y for f in flips]
    else:
        parts = [held]
    return parts, tuple(flips)


def body(normal_matrix, right_sides, tile_order, inner_order, block_lengths):
    f32 = jnp.float32
    tile = normal_matrix.shape[0]
    rhs = right_sides.shape[1]
    tiles = tile_order.shape[0]
    per_piece = rhs // (2 * tile // SUB)
    fit = sides_fit(tile, rhs)
    me = lax.axis_index(AXES).astype(jnp.int32).reshape(1)
    smem = pl.BlockSpec(memory_space=pltpu.SMEM)
    vmem = pl.BlockSpec(memory_space=pltpu.VMEM)
    hbm = pl.BlockSpec(memory_space=pl.ANY)
    shape = lambda *dims: jax.ShapeDtypeStruct(dims, f32)

    def held(*dims):
        return pltpu.VMEM(dims, f32) if small_enough(dims) else shape(*dims)

    def hold(x):
        return pltpu.with_memory_space_constraint(x, pltpu.VMEM) if small_enough(x.shape) else x


    slab_bytes = 4 * normal_matrix.size
    room = lambda slabs: pltpu.CompilerParams(vmem_limit_bytes=int(slabs * slab_bytes) + (4 << 20))

    small_rows = SUB if fit else 2 * SUB
    small = pl.pallas_call(
        near_body,
        out_shape=held(tiles * small_rows, tile),
        in_specs=[smem, smem, smem, vmem, hbm],
        out_specs=vmem,
        scratch_shapes=[pltpu.VMEM((2, tile, tile), f32), pltpu.SemaphoreType.DMA((2,))],
        name="near",
    )(me, tile_order, block_lengths, right_sides.T, normal_matrix)
    small_got = exchange(small, small_rows)
    tiles_out = pl.pallas_call(
        pack_body,
        out_shape=shape(tiles, tile, tile),
        in_specs=[smem, smem, vmem, vmem],
        out_specs=vmem,
        scratch_shapes=[pltpu.VMEM(normal_matrix.shape, f32)],
        name="pack",
    )(me, tile_order, inner_order, normal_matrix)
    routed_rows = MOSTT * SUB + (0 if fit else -(-MOSTT * per_piece // SUB) * SUB)
    routed = pl.pallas_call(
        lambda *refs: route_body(*refs, per_piece=per_piece),
        out_shape=held(tiles, routed_rows, tile),
        in_specs=[smem, smem, vmem],
        out_specs=vmem,
        scratch_shapes=[pltpu.SMEM((tiles + MOSTT,), jnp.int32)],
        name="route",
    )(tile_order, block_lengths, hold(small_got))
    block_parts = exchange(routed, routed_rows)
    tiles_got = exchange(tiles_out, tile)

    inverse_rows, own_sides, z = pl.pallas_call(
        lambda *refs: factor_body(*refs, per_piece=per_piece),
        out_shape=(held(MOSTT * tile, tile), held(rhs, tile), held(rhs, tile)),
        in_specs=[smem, smem, vmem, vmem],
        out_specs=(vmem, vmem, vmem),
        scratch_shapes=[
            pltpu.VMEM((MOSTT, tile, tile), f32),
            pltpu.VMEM((MOSTT, tile, tile), f32),
            pltpu.VMEM((MOSTT, rhs, tile), f32),
        ],
        name="factor",
        compiler_params=room(1),
    )(me, block_lengths, inner_order, hold(block_parts))

    iterate, flips = spread(z)
    slab = pl.pallas_call(
        arrange_body,
        out_shape=shape(tiles * tile, tile),
        in_specs=[smem, vmem],
        out_specs=hbm,
        scratch_shapes=[pltpu.SemaphoreType.DMA((tiles,))],
        name="arrange",
    compiler_params=room(1),
    )(tile_order, hold(tiles_got))

    def subtract(left, part, chosen):
        return pl.pallas_call(
            lambda *refs: residual_body(*refs, flips=chosen),
            out_shape=held(rhs, tile),
            in_specs=[smem, smem, vmem, vmem, vmem],
            out_specs=vmem,
            scratch_shapes=[
                pltpu.VMEM((rhs, len(chosen) * tile), f32),
                pltpu.VMEM((len(chosen) * tile, tile), f32),
            ],
            name="residual",
            compiler_params=room(3),
        )(me, tile_order, hold(tiles_got), hold(left), hold(part))

    residual = own_sides
    for part in iterate[:-1]:
        residual = subtract(residual, part, flips[: part.shape[0]])
        flips = flips[part.shape[0] :]
    residual = subtract(residual, iterate[-1], flips)
    near = [
        residual if o == 0 else shift(residual, -o) for o in range(1 - MOSTT, MOSTT)
    ]
    solved = pl.pallas_call(
        finish_body,
        out_shape=shape(rhs, tile),
        in_specs=[smem, smem, vmem, vmem] + [vmem] * len(near),
        out_specs=vmem,
        name="finish",
        compiler_params=room(0.5),
    )(me, block_lengths, hold(inverse_rows), hold(z), *map(hold, near))
    return slab, solved.T


def solution(mesh):
    placed = (P(AXES, None), P(AXES, None), P(), P(), P())
    return jax.shard_map(
        body,
        mesh=mesh,
        in_specs=placed,
        out_specs=(P(None, AXES), P(AXES, None)),
        check_vma=False,
    )
```
